32 devices in a mesh: ens: 2 (over y), gy: 4 (over z), gx: 4 (over x, core).
Axes of the slice: x: 2, y: 2, z: 4, core: 2. Of those that a mesh axis runs over, the one named last changes fastest.
Arguments:
- velocity: float32 [2, 2, 1024, 1024], P('ens', None, 'gy', 'gx'), may hold values from -3 to 3
- stress: float32 [2, 3, 1024, 1024], P('ens', None, 'gy', 'gx'), may hold values from -3 to 3
- thickness: float32 [2, 1024, 1024], P('ens', 'gy', 'gx'), may hold values from 2 to 3
- concentration: float32 [2, 1024, 1024], P('ens', 'gy', 'gx'), may hold values from 0.97 to 1
- node_mass: float32 [2, 1024, 1024], P('ens', 'gy', 'gx'), may hold values from 1 to 1.5
- wind_stress: float32 [2, 2, 1024, 1024], P('ens', None, 'gy', 'gx'), may hold values from -3 to 3
- ocean_current: float32 [2, 2, 1024, 1024], P('ens', None, 'gy', 'gx'), may hold values from -2 to 2
- ocean_mask: int32 [1024, 1024], P('gy', 'gx'), may hold values 0 or 1
- ice_blocks: int32 [2, 32, 32], P('ens', 'gy', 'gx'), may hold values 0 or 1
Outputs:
- velocity_out: float32 [2, 2, 1024, 1024], P('ens', None, 'gy', 'gx')
- stress_out: float32 [2, 3, 1024, 1024], P('ens', None, 'gy', 'gx')
- ensemble_mean: float32 [3, 1024, 1024], P(None, ('gy', 'ens'), 'gx')
- ensemble_variance: float32 [3, 1024, 1024], P(None, ('gy', 'ens'), 'gx')
The draws below stay inside these ranges and needn't reach their ends.
All inputs are finite; a program needn't handle non-finite values. No bound on the sum of `ocean_mask` or of `ice_blocks` on one device may be relied on, other than what follows from the above.
Results may differ from the reference program's by a relative error of at most 0.00002.
Values sent between devices are 32-bit elements; how exact they have to be, the bound alone decides.
A program may use at most 64 MiB of HBM per device.

```python
import math
import jax
import jax.numpy as jnp
from jax import lax

SUBCYCLES = 16
BLOCK = 32
MEMBERS = 2
NX = 1024
NY = 1024


def place_ends(entries, stream_key, low, high):
    extent = entries.shape
    place = [jax.random.randint(jax.random.fold_in(stream_key, axis), (), 0, extent[axis]) for axis in range(len(extent))]
    entries = entries.at[tuple(place)].set(low)
    longest = extent.index(max(extent))
    place[longest] = (place[longest] + 1) % extent[longest]
    return entries.at[tuple(place)].set(high)


def block_levels(key, dims, shards, smallest, largest):
    factor_of, own = 1.0, jax.random.fold_in(key, 6)
    for axis_at, shards_of in shards:
        draws = jnp.exp(jax.random.uniform(jax.random.fold_in(own, axis_at), (shards_of,), jnp.float32, smallest / len(shards), largest / len(shards)))
        factor_of = factor_of * jnp.repeat(draws, dims[axis_at] // shards_of).reshape([-1 if axis == axis_at else 1 for axis in range(len(dims))])
    return factor_of


def normal_values(rng, shape, scale, most, shards=(), kind=jnp.bfloat16):
    entries = jax.random.normal(rng, shape, jnp.float32) * scale
    if len(shards) > 0:
        entries = block_levels(rng, shape, shards, -0.22, 0.18) * entries
    return jnp.clip(entries, min=-most, max=most).astype(kind)


def setup_inputs(seed: int = 0) -> dict:
    key_list = jax.random.split(jax.random.key(seed), 10)
    return {
        "velocity": normal_values(key_list[0], (MEMBERS, 2, NY, NX), 0.5, 3.0, ((0, 2), (2, 4), (3, 4)), jnp.float32),
        "stress": normal_values(key_list[1], (MEMBERS, 3, NY, NX), 0.5, 3.0, ((0, 2), (2, 4), (3, 4)), jnp.float32),
        "thickness": jnp.clip(jnp.exp(math.log(3.0) - 0.4054651 * jax.random.uniform(key_list[2], (MEMBERS, NY, NX), jnp.float32) ** block_levels(key_list[2], (MEMBERS, NY, NX), ((0, 2), (1, 4), (2, 4)), -0.2, 0.2)), 2.0, 3.0),
        "concentration": jnp.clip(0.97 + 0.029999971 * jax.random.uniform(key_list[3], (MEMBERS, NY, NX), jnp.float32) ** block_levels(key_list[3], (MEMBERS, NY, NX), ((0, 2), (1, 4), (2, 4)), -0.2, 0.2), 0.97, 1.0),
        "node_mass": jnp.clip(jnp.exp(math.log(1.5) - 0.4054651 * jax.random.uniform(key_list[4], (MEMBERS, NY, NX), jnp.float32) ** block_levels(key_list[4], (MEMBERS, NY, NX), ((0, 2), (1, 4), (2, 4)), -0.2, 0.2)), 1.0, 1.5),
        "wind_stress": normal_values(key_list[5], (MEMBERS, 2, NY, NX), 0.5, 3.0, ((0, 2), (2, 4), (3, 4)), jnp.float32),
        "ocean_current": normal_values(key_list[6], (MEMBERS, 2, NY, NX), 0.3, 2.0, ((0, 2), (2, 4), (3, 4)), jnp.float32),
        "ocean_mask": place_ends((jax.random.randint(key_list[7], (NY, NX), 0, 5) < 4).astype(jnp.int32), jax.random.fold_in(key_list[7], 1), 0, 1),
        "ice_blocks": place_ends((jax.random.randint(key_list[8], (MEMBERS, NY // BLOCK, NX // BLOCK), 0, 4) < 3).astype(jnp.int32), jax.random.fold_in(key_list[8], 1), 0, 1),
    }


TIME_STEP = 0.5
RELAX_RATE = 0.25
ECCENTRICITY_SQUARED = 4.0
DELTA_FLOOR = 0.5
DRAG_WATER = 1.0
CORIOLIS_TOP = 1.0
STRENGTH_DECAY = 20.0
ADVECT_STEP = 1.0

def upper_extend(source):
    wrapped = jnp.concatenate([source, source[..., :1]], axis=-1)
    zeros_row = jnp.zeros_like(wrapped[..., :1, :])
    return jnp.concatenate([wrapped, zeros_row], axis=-2)

def lower_extend(source):
    wrapped = jnp.concatenate([source[..., -1:], source], axis=-1)
    zeros_row = jnp.zeros_like(wrapped[..., :1, :])
    return jnp.concatenate([zeros_row, wrapped], axis=-2)

def along_x(nodal_field):
    return 0.5 * (nodal_field[..., :-1, 1:] + nodal_field[..., 1:, 1:] - (nodal_field[..., :-1, :-1] + nodal_field[..., 1:, :-1]))

def along_y(nodal_field):
    return 0.5 * (nodal_field[..., 1:, :-1] + nodal_field[..., 1:, 1:] - (nodal_field[..., :-1, :-1] + nodal_field[..., :-1, 1:]))

def stress_update(stresses, extended_vel, strength):
    divergence = along_x(extended_vel[:, 0]) + along_y(extended_vel[:, 1])
    tension = along_x(extended_vel[:, 0]) - along_y(extended_vel[:, 1])
    shearing = along_y(extended_vel[:, 0]) + along_x(extended_vel[:, 1])
    deform = jnp.sqrt(divergence * divergence + (tension * tension + shearing * shearing) / ECCENTRICITY_SQUARED)
    bounded = jnp.maximum(deform, DELTA_FLOOR)
    weight = RELAX_RATE * 0.5 * strength / bounded
    stress_one = (stresses[:, 0] + weight * (divergence - deform)) / (1.0 + RELAX_RATE)
    stress_two = (stresses[:, 1] + weight * tension / ECCENTRICITY_SQUARED) / (1.0 + RELAX_RATE)
    stress_three = (stresses[:, 2] + weight * shearing / (2.0 * ECCENTRICITY_SQUARED)) / (1.0 + RELAX_RATE)
    return jnp.stack([stress_one, stress_two, stress_three], axis=1)

def momentum_update(moving, extended_stress, node_mass, wind_stress, ocean_current, coriolis, active):
    normal_east = 0.5 * (extended_stress[:, 0] + extended_stress[:, 1])
    normal_north = 0.5 * (extended_stress[:, 0] - extended_stress[:, 1])
    shear_part = extended_stress[:, 2]
    force_east = along_x(normal_east) + along_y(shear_part)
    force_north = along_x(shear_part) + along_y(normal_north)
    east_vel = moving[:, 0]
    north_vel = moving[:, 1]
    current_east = ocean_current[:, 0]
    current_north = ocean_current[:, 1]
    drag_rate = DRAG_WATER * jnp.sqrt((current_east - east_vel) * (current_east - east_vel) + (current_north - north_vel) * (current_north - north_vel))
    inertia = node_mass / TIME_STEP
    diagonal_term = inertia + drag_rate
    turning = coriolis * node_mass
    rhs_east = inertia * east_vel + force_east + wind_stress[:, 0] + drag_rate * current_east
    rhs_north = inertia * north_vel + force_north + wind_stress[:, 1] + drag_rate * current_north
    determinant = diagonal_term * diagonal_term + turning * turning
    new_east = active * (diagonal_term * rhs_east + turning * rhs_north) / determinant
    new_north = active * (diagonal_term * rhs_north - turning * rhs_east) / determinant
    return jnp.stack([new_east, new_north], axis=1)

def reference(velocity, stress, thickness, concentration, node_mass, wind_stress, ocean_current, ocean_mask, ice_blocks):
    present = jnp.repeat(jnp.repeat(ice_blocks, BLOCK, axis=1), BLOCK, axis=2).astype(jnp.float32)
    active = ocean_mask.astype(jnp.float32)[None] * present
    strength = thickness * jnp.exp(-STRENGTH_DECAY * (1.0 - concentration))
    row_index = jnp.arange(NY, dtype=jnp.int32).astype(jnp.float32)
    coriolis = (CORIOLIS_TOP * (row_index + 0.5) / NY)[:, None]
    initial = velocity * active[:, None]

    def subcycle(counter, carried):
        moving, stresses = carried
        stresses = stress_update(stresses, upper_extend(moving), strength)
        moving = momentum_update(moving, lower_extend(stresses), node_mass, wind_stress, ocean_current, coriolis, active)
        return (moving, stresses)
    final_vel, final_stress = lax.fori_loop(0, SUBCYCLES, subcycle, (initial, stress))
    extended = upper_extend(final_vel)
    divergence = along_x(extended[:, 0]) + along_y(extended[:, 1])
    drifted = jnp.clip(concentration - ADVECT_STEP * concentration * divergence, 0.0, 1.0)
    fields = jnp.stack([drifted, final_vel[:, 0], final_vel[:, 1]], axis=1)
    average = lax.optimization_barrier(jnp.sum(fields, axis=0)) / MEMBERS
    deviation = fields - average[None]
    spread = lax.optimization_barrier(jnp.sum(deviation * deviation, axis=0)) / MEMBERS
    return (final_vel, final_stress, average, spread)
```

```python
import functools

import jax
import jax.numpy as jnp
from jax import lax
from jax.experimental import pallas as pl
from jax.experimental.pallas import tpu as pltpu
from jax.sharding import PartitionSpec as P

SUBCYCLES = 16
BLOCK = 32

TIME_STEP = 0.5
RELAX_RATE = 0.25
ECCENTRICITY_SQUARED = 4.0
CORIOLIS_TOP = 1.0
STRENGTH_DECAY = 20.0

MESH = pl.DeviceIdType.MESH
LANES = 128
TINY = 1.1754944e-38
GAIN = 1.0 + RELAX_RATE

MARGIN = SUBCYCLES
EXTRA = 8
TOP = 8
LOW = TOP
MID = TOP + MARGIN
STEP = 16

PACKED = (
    ("u", MARGIN + 1), ("v", MARGIN + 1), ("plus", MARGIN), ("minus", MARGIN), ("twice", MARGIN),
    ("pressure", MARGIN), ("inertia", MARGIN),
    ("ge", MARGIN), ("gn", MARGIN), ("ce", MARGIN), ("cn", MARGIN),
)
WHOLE = 7
OFFSETS = []
for _i, (_, _w) in enumerate(PACKED):
    if _i == 0 or _i == WHOLE:
        OFFSETS.append(0)
    else:
        OFFSETS.append(OFFSETS[-1] + PACKED[_i - 1][1])
HALF = LANES // 2

OWN = 36
AT_LEFT = MARGIN
AT_RIGHT = MARGIN + OWN
AT_HALO = MARGIN + 2 * OWN
AT_END = AT_HALO + MARGIN + 1

MAIN_FIELDS = (
    "u", "v", "plus", "minus", "twice", "pressure", "inertia", "turning",
    "ge", "gn", "ce", "cn", "cae", "can", "active",
)


def lane_index(rows):
    return lax.broadcasted_iota(jnp.int32, (rows, LANES), 1)


def rolled(value, shift):
    shift = shift % LANES
    return value if shift == 0 else pltpu.roll(value, shift, 1)


def step_kernel(sizes, *refs):
    gx_count, gy_count, ens_count = sizes
    inputs, refs = refs[:9], refs[9:]
    (vel_out, stress_out, conc_out, landing), refs = refs[:4], refs[4:]
    (svel, sstress, sthick, sconc, smass, swind, scur, smask, sice, expand), refs = refs[:10], refs[10:]
    arrays, refs = refs[: len(MAIN_FIELDS)], refs[len(MAIN_FIELDS) :]
    (out_a, out_b, in_a, in_b, load_sem, send_y, recv_y, send_x, recv_x, send_d, recv_d, send_e, recv_e) = refs
    field = dict(zip(MAIN_FIELDS, arrays))
    stages = (svel, sstress, sthick, sconc, smass, swind, scur, smask)
    rows, cols = conc_out.shape
    main = cols // LANES
    tiles = main + 1
    high = MID + rows
    blocks = rows // BLOCK
    gx, gy, me = lax.axis_index("gx"), lax.axis_index("gy"), lax.axis_index("ens")
    right, left = lax.rem(gx + 1, gx_count), lax.rem(gx + gx_count - 1, gx_count)
    has_lo, has_hi = gy > 0, gy < gy_count - 1
    lower, upper = jnp.maximum(gy - 1, 0), jnp.minimum(gy + 1, gy_count - 1)
    peers = [lax.rem(me + step, ens_count) for step in range(1, ens_count)]

    barrier = pltpu.get_barrier_semaphore()

    def greet(**where):
        pl.semaphore_signal(barrier, inc=1, device_id=where, device_id_type=MESH)

    greet(gx=left)
    greet(gx=right)
    for peer in peers:
        greet(ens=peer)
    for there, row in ((has_lo, lower), (has_hi, upper)):
        @pl.when(there)
        def _(row=row):
            greet(gy=row)
            greet(gy=row, gx=left)
            greet(gy=row, gx=right)

    own = slice(MARGIN, MARGIN + rows)

    def at_rows(ref, where):
        return ref.at[:, where] if len(ref.shape) == 3 else ref.at[where]

    loads = [
        pltpu.make_async_copy(source, at_rows(stage, own), load_sem.at[number])
        for number, (source, stage) in enumerate(zip(inputs, stages))
    ]
    loads.append(pltpu.make_async_copy(inputs[8], sice.at[blocks : 2 * blocks], load_sem.at[8]))
    for each in loads:
        each.start()

    def remote(source, target, sends, receives, number, where):
        return pltpu.make_async_remote_copy(
            src_ref=source, dst_ref=target, send_sem=sends.at[number], recv_sem=receives.at[number],
            device_id=where, device_id_type=MESH,
        )

    down, up = [], []
    for number, (source, stage) in enumerate(zip(inputs, stages)):
        extra = EXTRA if number in (0, 7) else 0
        down.append(remote(
            at_rows(source, slice(0, MARGIN + extra)),
            at_rows(stage, slice(MARGIN + rows, 2 * MARGIN + rows + extra)),
            send_y, recv_y, number, {"gy": lower},
        ))
        up.append(remote(
            at_rows(source, slice(rows - MARGIN, rows)),
            at_rows(stage, slice(0, MARGIN)),
            send_y, recv_y, 9 + number, {"gy": upper},
        ))
    down.append(remote(inputs[8], sice.at[2 * blocks : 3 * blocks], send_y, recv_y, 8, {"gy": lower}))
    up.append(remote(inputs[8], sice.at[0:blocks], send_y, recv_y, 17, {"gy": upper}))

    others = has_lo.astype(jnp.int32) + has_hi.astype(jnp.int32)
    pl.semaphore_wait(barrier, 2 + (ens_count - 1) + 3 * others)

    @pl.when(has_lo)
    def _():
        for each in down:
            each.start()

    @pl.when(has_hi)
    def _():
        for each in up:
            each.start()

    for each in loads:
        each.wait()

    block_cols = sice.shape[1]
    spread = (
        lax.broadcasted_iota(jnp.int32, (block_cols, cols), 1) // BLOCK
        == lax.broadcasted_iota(jnp.int32, (block_cols, cols), 0)
    ).astype(jnp.float32)

    repeat = (
        lax.broadcasted_iota(jnp.int32, (8 * blocks, blocks), 0) // 8
        == lax.broadcasted_iota(jnp.int32, (8 * blocks, blocks), 1)
    ).astype(jnp.float32)

    def expand_ice(part):
        flags = sice[part * blocks : (part + 1) * blocks].astype(jnp.float32)
        flags = jnp.dot(repeat, flags, preferred_element_type=jnp.float32)
        expand[8 * part * blocks : 8 * (part + 1) * blocks] = jnp.dot(
            flags, spread, preferred_element_type=jnp.float32)

    def convert(start, count, ice_row):
        at = pl.ds(start, count)
        to = pl.ds(start + TOP, count)
        row = lax.broadcasted_iota(jnp.int32, (count, LANES), 0) + (gy * rows + (start - MARGIN))
        coriolis = CORIOLIS_TOP * (row.astype(jnp.float32) + 0.5) / (rows * gy_count)
        for t in range(main):
            c = slice(t * LANES, (t + 1) * LANES)
            present = jnp.concatenate([expand[pl.ds(ice_row, 8), c]] * (count // 8))
            alive = smask[at, c].astype(jnp.float32) * present
            field["active"][t, to] = alive
            field["u"][t, to] = svel[0, at, c] * alive
            field["v"][t, to] = svel[1, at, c] * alive
            one, two = sstress[0, at, c], sstress[1, at, c]
            field["plus"][t, to] = one + two
            field["minus"][t, to] = one - two
            field["twice"][t, to] = 2.0 * sstress[2, at, c]
            factor = RELAX_RATE * 0.5 / GAIN
            field["pressure"][t, to] = factor * sthick[at, c] * jnp.exp(-STRENGTH_DECAY * (1.0 - sconc[at, c]))
            heavy = smass[at, c]
            heavy = jnp.where(heavy == 0.0, 1.0, heavy)
            turn = coriolis * heavy
            ce, cn = scur[0, at, c], scur[1, at, c]
            field["inertia"][t, to] = heavy / TIME_STEP
            field["turning"][t, to] = turn
            field["ge"][t, to] = swind[0, at, c] + turn * cn
            field["gn"][t, to] = swind[1, at, c] - turn * ce
            field["ce"][t, to] = ce
            field["cn"][t, to] = cn
            field["cae"][t, to] = alive * ce
            field["can"][t, to] = alive * cn

    expand_ice(1)

    def convert_own(block, _):
        convert(pl.multiple_of(MARGIN + block * BLOCK, 8), BLOCK, pl.multiple_of(8 * (blocks + block), 8))
        return 0

    lax.fori_loop(0, blocks, convert_own, 0)

    def message(name, tile, at):
        value = field[name][tile, at]
        return value * field["active"][tile, at] if name == "inertia" else value

    def packed(fields, at, count):
        lanes = lane_index(count)
        east = jnp.zeros((count, LANES), jnp.float32)
        west = jnp.zeros((count, LANES), jnp.float32)
        for number in fields:
            name, width = PACKED[number]
            start = OFFSETS[number]
            here = jnp.logical_and(lanes >= start, lanes < start + width)
            east = jnp.where(here, rolled(message(name, main - 1, at), start - (LANES - MARGIN)), east)
            west = jnp.where(here, rolled(message(name, 0, at), start), west)
        return east, west

    whole, part = range(WHOLE), range(WHOLE, len(PACKED))

    def pack_own(block, _):
        start = pl.multiple_of(block * BLOCK, 8)
        east, west = packed(whole, pl.ds(MID + start, BLOCK), BLOCK)
        out_a[0, pl.ds(start, BLOCK)] = east
        out_a[1, pl.ds(start, BLOCK)] = west
        return 0

    lax.fori_loop(0, blocks, pack_own, 0)

    def pack_half(block, _):
        start = pl.multiple_of(block * BLOCK, 8)
        east, west = packed(part, pl.ds(MID + start, BLOCK), BLOCK)
        more_east, more_west = packed(part, pl.ds(MID + rows // 2 + start, BLOCK), BLOCK)
        second = lane_index(BLOCK) >= HALF
        out_b[0, pl.ds(start, BLOCK)] = jnp.where(second, rolled(more_east, HALF), east)
        out_b[1, pl.ds(start, BLOCK)] = jnp.where(second, rolled(more_west, HALF), west)
        return 0

    lax.fori_loop(0, blocks // 2, pack_half, 0)

    sides = (right, left)
    across, corner_lo, corner_hi = [], [], []
    half_rows = rows // 2
    for side, to in enumerate(sides):
        across.append(remote(
            out_a.at[side], in_a.at[side, MARGIN : MARGIN + rows], send_x, recv_x, 2 * side, {"gx": to}))
        across.append(remote(
            out_b.at[side], in_b.at[side, MARGIN : MARGIN + half_rows], send_x, recv_x, 2 * side + 1, {"gx": to}))
        lo, hi = {"gx": to, "gy": lower}, {"gx": to, "gy": upper}
        corner_lo.append(remote(
            out_a.at[side, 0 : MARGIN + EXTRA],
            in_a.at[side, MARGIN + rows : 2 * MARGIN + rows + EXTRA],
            send_d, recv_d, 4 * side, lo))
        corner_lo.append(remote(
            out_b.at[side, 0:MARGIN],
            in_b.at[side, MARGIN + half_rows : 2 * MARGIN + half_rows],
            send_d, recv_d, 4 * side + 1, lo))
        corner_hi.append(remote(
            out_a.at[side, rows - MARGIN : rows], in_a.at[side, 0:MARGIN],
            send_d, recv_d, 4 * side + 2, hi))
        corner_hi.append(remote(
            out_b.at[side, half_rows - MARGIN : half_rows], in_b.at[side, 0:MARGIN],
            send_d, recv_d, 4 * side + 3, hi))
    for each in across:
        each.start()

    @pl.when(has_lo)
    def _():
        for each in corner_lo:
            each.start()

    @pl.when(has_hi)
    def _():
        for each in corner_hi:
            each.start()

    @pl.when(has_lo)
    def _():
        for each in up:
            each.wait_recv()

    @pl.when(jnp.logical_not(has_lo))
    def _():
        for stage in stages:
            for index in range(stage.shape[0]) if len(stage.shape) == 3 else (None,):
                view = stage if index is None else stage.at[index]
                view[0:MARGIN] = jnp.zeros((MARGIN, cols), stage.dtype)
        sice[0:blocks] = jnp.zeros((blocks, block_cols), jnp.int32)

    @pl.when(has_hi)
    def _():
        for each in down:
            each.wait_recv()

    @pl.when(jnp.logical_not(has_hi))
    def _():
        for stage in stages:
            count = stage.shape[-2] - MARGIN - rows
            for index in range(stage.shape[0]) if len(stage.shape) == 3 else (None,):
                view = stage if index is None else stage.at[index]
                view[MARGIN + rows : MARGIN + rows + count] = jnp.zeros((count, cols), stage.dtype)
        sice[2 * blocks : 3 * blocks] = jnp.zeros((blocks, block_cols), jnp.int32)

    expand_ice(0)
    expand_ice(2)
    convert(0, MARGIN, 8 * (blocks - 1))
    convert(MARGIN + rows, MARGIN, 16 * blocks)
    beyond = slice(2 * MARGIN + rows, 2 * MARGIN + rows + EXTRA)
    past = slice(high + MARGIN, high + MARGIN + EXTRA)
    for t in range(main):
        c = slice(t * LANES, (t + 1) * LANES)
        alive = smask[beyond, c].astype(jnp.float32) * expand[16 * blocks : 16 * blocks + 8, c]
        field["u"][t, past] = svel[0, beyond, c] * alive
        field["v"][t, past] = svel[1, beyond, c] * alive

    for each in across:
        each.wait_recv()

    @pl.when(has_lo)
    def _():
        for each in corner_hi:
            each.wait_recv()

    @pl.when(jnp.logical_not(has_lo))
    def _():
        for side in range(2):
            in_a[side, 0:MARGIN] = jnp.zeros((MARGIN, LANES), jnp.float32)
            in_b[side, 0:MARGIN] = jnp.zeros((MARGIN, LANES), jnp.float32)

    @pl.when(has_hi)
    def _():
        for each in corner_lo:
            each.wait_recv()

    @pl.when(jnp.logical_not(has_hi))
    def _():
        for side in range(2):
            in_a[side, MARGIN + rows :] = jnp.zeros((MARGIN + EXTRA, LANES), jnp.float32)
            in_b[side, MARGIN + half_rows :] = jnp.zeros((MARGIN, LANES), jnp.float32)

    def strip_value(number, start, count, half_start, half_lane):
        name, width = PACKED[number]
        lanes = lane_index(count)
        at = pl.ds(start, count)
        if number < WHOLE:
            arrived, there, lane = in_a, pl.ds(start - TOP, count), OFFSETS[number]
        else:
            arrived, there, lane = in_b, pl.ds(half_start, count), OFFSETS[number] + half_lane
        value = jnp.where(lanes < AT_HALO, rolled(message(name, main - 1, at), AT_HALO - LANES),
                          rolled(arrived[1, there], AT_HALO - lane))
        value = jnp.where(lanes < AT_RIGHT, rolled(message(name, 0, at), AT_LEFT), value)
        value = jnp.where(lanes < AT_LEFT, rolled(arrived[0, there], -lane), value)
        return jnp.where(lanes < AT_HALO + width, value, 0.0)

    def strip_rows(start, count, half_start, half_lane):
        at = pl.ds(start, count)
        value = {
            name: strip_value(number, start, count, half_start, half_lane)
            for number, (name, _) in enumerate(PACKED)
        }
        row = lax.broadcasted_iota(jnp.int32, (count, LANES), 0) + (gy * rows + (start - MID))
        coriolis = CORIOLIS_TOP * (row.astype(jnp.float32) + 0.5) / (rows * gy_count)
        empty = value["inertia"] == 0.0
        alive = jnp.where(empty, 0.0, 1.0)
        heavy = jnp.where(empty, 1.0 / TIME_STEP, value["inertia"])
        value["inertia"] = heavy
        value["turning"] = coriolis * (heavy * TIME_STEP)
        value["active"] = alive
        value["cae"] = alive * value["ce"]
        value["can"] = alive * value["cn"]
        for name in MAIN_FIELDS:
            field[name][main, at] = value[name]

    for half in range(2):
        def strip_own(block, _, half=half):
            start = pl.multiple_of(block * BLOCK, 8)
            strip_rows(MID + half * half_rows + start, BLOCK, MARGIN + start, half * HALF)
            return 0

        lax.fori_loop(0, blocks // 2, strip_own, 0)
    strip_rows(LOW, MARGIN, 0, HALF)
    strip_rows(high, MARGIN, MARGIN + half_rows, 0)
    for number in range(2):
        field[PACKED[number][0]][main, past] = strip_value(number, high + MARGIN, EXTRA, 0, 0)
    for name in ("plus", "minus", "twice"):
        for t in range(tiles):
            field[name][t, 0:LOW] = jnp.zeros((LOW, LANES), jnp.float32)

    u, v, plus, minus, twice = (field[name] for name in ("u", "v", "plus", "minus", "twice"))
    lanes = lane_index(STEP)
    at_end, at_start = lanes == LANES - 1, lanes == 0

    def ahead(values):
        turned = [rolled(value, -1) for value in values]
        return [jnp.where(at_end, turned[(t + 1) % main], turned[t]) for t in range(main)] + turned[main:]

    def behind(values):
        turned = [rolled(value, 1) for value in values]
        return [jnp.where(at_start, turned[t - 1 if t else main - 1], turned[t]) for t in range(main)] + turned[main:]

    def gradients(start):
        add, sub, add_s, sub_s = [], [], [], []
        for t in range(tiles):
            u0, u1 = u[t, pl.ds(start, STEP)], u[t, pl.ds(start + 1, STEP)]
            v0, v1 = v[t, pl.ds(start, STEP)], v[t, pl.ds(start + 1, STEP)]
            a, b, c, d = u0 + u1, u1 - u0, v0 + v1, v1 - v0
            add.append(a + d)
            sub.append(a - d)
            add_s.append(b + c)
            sub_s.append(b - c)
        return add, sub, add_s, sub_s

    def stress_rows(start, growth):
        at = pl.ds(start, STEP)
        add, sub, add_s, sub_s = gradients(start)
        add_next, sub_next, shear_next = ahead(add), ahead(sub), ahead(add_s)
        for t in range(tiles):
            div = add_next[t] - sub[t]
            tension = sub_next[t] - add[t]
            shear = shear_next[t] + sub_s[t]
            square = div * div + (1.0 / ECCENTRICITY_SQUARED) * (tension * tension + shear * shear)
            inverse = lax.rsqrt(jnp.maximum(square, TINY))
            ratio = jnp.minimum(square * inverse, 1.0)
            force = field["pressure"][t, at] * growth
            weight = force * jnp.minimum(inverse, 1.0)
            quarter = weight * (1.0 / ECCENTRICITY_SQUARED)
            change = weight * div - force * ratio
            other = quarter * tension
            plus[t, at] = plus[t, at] + (change + other)
            minus[t, at] = minus[t, at] + (change - other)
            twice[t, at] = twice[t, at] + quarter * shear

    def velocity_rows(start, scale):
        at, before = pl.ds(start, STEP), pl.ds(start - 1, STEP)
        e_near, e_far, n_near, n_far = [], [], [], []
        for t in range(tiles):
            p1, p0 = plus[t, at], plus[t, before]
            m1, m0 = minus[t, at], minus[t, before]
            s1, s0 = twice[t, at], twice[t, before]
            a, d, b, e = p0 + p1, s1 - s0, s0 + s1, m1 - m0
            e_near.append(a + d)
            e_far.append(a - d)
            n_near.append(b + e)
            n_far.append(b - e)
        e_far, n_far = behind(e_far), behind(n_far)
        for t in range(tiles):
            de, dn = u[t, at] - field["ce"][t, at], v[t, at] - field["cn"][t, at]
            square = de * de + dn * dn
            drag = square * lax.rsqrt(jnp.maximum(square, TINY))
            heavy, turn = field["inertia"][t, at], field["turning"][t, at]
            diag = heavy + drag
            push_e = heavy * de + ((e_near[t] - e_far[t]) * scale + field["ge"][t, at])
            push_n = heavy * dn + ((n_near[t] - n_far[t]) * scale + field["gn"][t, at])
            inverse = lax.rsqrt(diag * diag + turn * turn)
            inverse = field["active"][t, at] * (inverse * inverse)
            u[t, at] = (diag * push_e + turn * push_n) * inverse + field["cae"][t, at]
            v[t, at] = (diag * push_n - turn * push_e) * inverse + field["can"][t, at]

    count = (high + MARGIN - LOW) // STEP

    def subcycle(_, carried):
        growth, scale = carried
        stress_rows(LOW, growth)

        def both(block, _):
            start = pl.multiple_of(LOW + block * STEP, 8)
            stress_rows(start, growth)
            velocity_rows(start - STEP, scale)
            return 0

        lax.fori_loop(1, count, both, 0)
        velocity_rows(LOW + (count - 1) * STEP, scale)
        return growth * GAIN, scale * (1.0 / GAIN)

    lax.fori_loop(0, SUBCYCLES, subcycle, (jnp.float32(GAIN), jnp.float32(0.25 / GAIN)))

    shrink = 0.5 * GAIN**-SUBCYCLES
    on_left, on_right = lanes < MARGIN, lanes >= LANES - MARGIN - 2

    def merged(values):
        values = list(values)
        values[0] = jnp.where(on_left, rolled(values[main], -AT_LEFT), values[0])
        values[main - 1] = jnp.where(on_right, rolled(values[main], LANES - AT_HALO), values[main - 1])
        return values[:main]

    def finish(block, _):
        start = pl.multiple_of(block * STEP, 8)
        here, at = pl.ds(MID + start, STEP), pl.ds(start, STEP)
        add, sub, _, _ = gradients(MID + start)
        add_next = ahead(add)
        div = merged([add_next[t] - sub[t] for t in range(tiles)])
        east, north, one, two, three = (
            merged([ref[t, here] for t in range(tiles)]) for ref in (u, v, plus, minus, twice)
        )
        for t in range(main):
            c = slice(t * LANES, (t + 1) * LANES)
            vel_out[0, at, c] = east[t]
            vel_out[1, at, c] = north[t]
            stress_out[0, at, c] = (one[t] + two[t]) * shrink
            stress_out[1, at, c] = (one[t] - two[t]) * shrink
            stress_out[2, at, c] = three[t] * shrink
            value = sconc[pl.ds(MARGIN + start, STEP), c]
            conc_out[at, c] = jnp.clip(value - value * (0.5 * div[t]), 0.0, 1.0)
        return 0

    lax.fori_loop(0, rows // STEP, finish, 0)

    share = rows // ens_count
    swaps = []
    for step, peer in enumerate(peers):
        part_of = pl.ds(pl.multiple_of(peer * share, 8), share)
        swaps.append(remote(
            conc_out.at[part_of], landing.at[step, 0], send_e, recv_e, 2 * step, {"ens": peer}))
        swaps.append(remote(
            vel_out.at[:, part_of], landing.at[step, 1:3], send_e, recv_e, 2 * step + 1, {"ens": peer}))
    for each in swaps:
        each.start()
    for each in across:
        each.wait_send()

    @pl.when(has_lo)
    def _():
        for each in down + corner_lo:
            each.wait_send()

    @pl.when(has_hi)
    def _():
        for each in up + corner_hi:
            each.wait_send()

    for each in swaps:
        each.wait_recv()
    for each in swaps:
        each.wait_send()


def write_kernel(count, vel, stress, conc, landing, vel_out, stress_out, mean_out, spread_out, mean, spread, sems):
    copies = [
        pltpu.make_async_copy(vel, vel_out, sems.at[0]),
        pltpu.make_async_copy(stress, stress_out, sems.at[1]),
    ]
    for each in copies:
        each.start()
    share = mean.shape[1]
    own = pl.ds(pl.multiple_of(lax.axis_index("ens") * share, 8), share)
    for f in range(3):
        values = [conc[own] if f == 0 else vel[f - 1, own]]
        values += [landing[step, f] for step in range(count - 1)]
        average = functools.reduce(jnp.add, values) / count
        mean[f] = average
        spread[f] = functools.reduce(jnp.add, [(v - average) * (v - average) for v in values]) / count
    more = [
        pltpu.make_async_copy(mean, mean_out, sems.at[2]),
        pltpu.make_async_copy(spread, spread_out, sems.at[3]),
    ]
    for each in more:
        each.start()
    for each in copies + more:
        each.wait()


def solution(mesh):
    gx_count, gy_count, ens_count = mesh.shape["gx"], mesh.shape["gy"], mesh.shape["ens"]
    f32 = jnp.float32

    def vmem(*shape, dtype=f32):
        return pltpu.VMEM(shape, dtype)

    def specs(count, space):
        return [pl.BlockSpec(memory_space=space)] * count

    def body(velocity, stress, thickness, concentration, node_mass, wind, current, mask, ice):
        rows, cols = mask.shape
        share = rows // ens_count
        tiles = cols // LANES + 1
        block_rows, block_cols = ice.shape[1:]
        tall = rows + 2 * MARGIN
        total = TOP + tall + EXTRA
        shape = lambda *dims: jax.ShapeDtypeStruct(dims, f32)
        dma = lambda count: pltpu.SemaphoreType.DMA((count,))
        state = pl.pallas_call(
            functools.partial(step_kernel, (gx_count, gy_count, ens_count)),
            name="subcycles",
            out_shape=(
                shape(2, rows, cols),
                shape(3, rows, cols),
                shape(rows, cols),
                shape(ens_count - 1, 3, share, cols),
            ),
            in_specs=specs(9, pltpu.HBM),
            out_specs=tuple(specs(4, pltpu.VMEM)),
            scratch_shapes=[
                vmem(2, tall + EXTRA, cols),
                vmem(3, tall, cols),
                vmem(tall, cols),
                vmem(tall, cols),
                vmem(tall, cols),
                vmem(2, tall, cols),
                vmem(2, tall, cols),
                vmem(tall + EXTRA, cols, dtype=jnp.int32),
                vmem(3 * block_rows, block_cols, dtype=jnp.int32),
                vmem(24 * block_rows, cols),
            ]
            + [vmem(tiles, total, LANES)] * len(MAIN_FIELDS)
            + [
                vmem(2, rows, LANES),
                vmem(2, rows // 2, LANES),
                vmem(2, tall + EXTRA, LANES),
                vmem(2, rows // 2 + 2 * MARGIN, LANES),
                dma(9), dma(18), dma(18), dma(4), dma(4), dma(8), dma(8),
                dma(2 * (ens_count - 1)), dma(2 * (ens_count - 1)),
            ],
            compiler_params=pltpu.CompilerParams(
                collective_id=0, has_side_effects=True, vmem_limit_bytes=24 << 20),
        )(*(pltpu.with_memory_space_constraint(each, pltpu.HBM) for each in (
            velocity[0], stress[0], thickness[0], concentration[0], node_mass[0], wind[0], current[0], mask, ice[0])))
        vel_out, stress_out, mean, spread = pl.pallas_call(
            functools.partial(write_kernel, ens_count),
            name="write",
            out_shape=(shape(2, rows, cols), shape(3, rows, cols), shape(3, share, cols), shape(3, share, cols)),
            in_specs=specs(4, pltpu.VMEM),
            out_specs=tuple(specs(4, pltpu.HBM)),
            scratch_shapes=[vmem(3, share, cols), vmem(3, share, cols), dma(4)],
            compiler_params=pltpu.CompilerParams(vmem_limit_bytes=4 << 20),
        )(*state)
        return vel_out[None], stress_out[None], mean, spread

    grid = P("ens", "gy", "gx")
    pair = P("ens", None, "gy", "gx")
    split = P(None, ("gy", "ens"), "gx")
    return jax.shard_map(
        body,
        mesh=mesh,
        in_specs=(pair, pair, grid, grid, grid, pair, pair, P("gy", "gx"), grid),
        out_specs=(pair, pair, split, split),
        check_vma=False,
    )
```

```python
import functools

import jax
import jax.numpy as jnp
from jax import lax
from jax.experimental import pallas as pl
from jax.experimental.pallas import tpu as pltpu
from jax.sharding import PartitionSpec as P

SUBCYCLES = 16
BLOCK = 32

TIME_STEP = 0.5
RELAX_RATE = 0.25
ECCENTRICITY_SQUARED = 4.0
CORIOLIS_TOP = 1.0
STRENGTH_DECAY = 20.0

MESH = pl.DeviceIdType.MESH
LANES = 128
TINY = 1.1754944e-38
GAIN = 1.0 + RELAX_RATE

MARGIN = SUBCYCLES
EXTRA = 8
PAD = 8
STEP = 32

PACKED = (
    ("u", MARGIN + 1), ("v", MARGIN + 1), ("plus", MARGIN), ("minus", MARGIN), ("twice", MARGIN),
    ("pressure", MARGIN), ("inertia", MARGIN),
    ("ge", MARGIN), ("gn", MARGIN), ("ce", MARGIN), ("cn", MARGIN),
)
WHOLE = 7
OFFSETS = []
for _i, (_, _w) in enumerate(PACKED):
    if _i == 0 or _i == WHOLE:
        OFFSETS.append(0)
    else:
        OFFSETS.append(OFFSETS[-1] + PACKED[_i - 1][1])
HALF = LANES // 2

OWN = 36
AT_RIGHT = 48
AT_HALO = AT_RIGHT + OWN
AT_LEFT = LANES - MARGIN

MAIN_FIELDS = (
    "u", "v", "plus", "minus", "twice", "pressure", "inertia", "turning",
    "ge", "gn", "ce", "cn", "cae", "can", "bound",
    "add", "sub", "sub_s", "add_next", "sub_next", "shear_next", "e_near", "n_near", "e_back", "n_back",
)


def lane_index(rows):
    return lax.broadcasted_iota(jnp.int32, (rows, LANES), 1)


def rolled(value, shift):
    shift = shift % LANES
    return value if shift == 0 else pltpu.roll(value, shift, 1)


def step_kernel(sizes, *refs):
    gx_count, gy_count, ens_count = sizes
    inputs, refs = refs[:9], refs[9:]
    (vel_out, stress_out, conc_out, landing), refs = refs[:4], refs[4:]
    arrays, refs = refs[: len(MAIN_FIELDS)], refs[len(MAIN_FIELDS) :]
    (svel, sstress, sthick, sconc, smass, swind, scur, smask, sice, expand), refs = refs[:10], refs[10:]
    (out_a, out_b, in_a, in_b, load_sem, send_y, recv_y, send_x, recv_x, send_d, recv_d, send_e, recv_e) = refs
    field = dict(zip(MAIN_FIELDS, arrays))
    stages = (svel, sstress, sthick, sconc, smass, swind, scur, smask)
    rows, cols = conc_out.shape
    main = cols // LANES
    tiles = main + 1
    blocks = rows // BLOCK
    half_rows = rows // 2
    reach = half_rows + 2 * MARGIN
    bases = (PAD, 3 * PAD + reach)
    first_rows = (-MARGIN, half_rows - MARGIN)
    spare = 5 * PAD + 2 * reach
    gx, gy, me = lax.axis_index("gx"), lax.axis_index("gy"), lax.axis_index("ens")
    right, left = lax.rem(gx + 1, gx_count), lax.rem(gx + gx_count - 1, gx_count)
    has_lo, has_hi = gy > 0, gy < gy_count - 1
    lower, upper = jnp.maximum(gy - 1, 0), jnp.minimum(gy + 1, gy_count - 1)
    peers = [lax.rem(me + step, ens_count) for step in range(1, ens_count)]

    barrier = pltpu.get_barrier_semaphore()

    def greet(**where):
        pl.semaphore_signal(barrier, inc=1, device_id=where, device_id_type=MESH)

    greet(gx=left)
    greet(gx=right)
    for peer in peers:
        greet(ens=peer)
    for there, row in ((has_lo, lower), (has_hi, upper)):
        @pl.when(there)
        def _(row=row):
            greet(gy=row)
            greet(gy=row, gx=left)
            greet(gy=row, gx=right)

    own = slice(MARGIN, MARGIN + rows)

    def at_rows(ref, where):
        return ref.at[:, where] if len(ref.shape) == 3 else ref.at[where]

    loads = [
        pltpu.make_async_copy(source, at_rows(stage, own), load_sem.at[number])
        for number, (source, stage) in enumerate(zip(inputs, stages))
    ]
    loads.append(pltpu.make_async_copy(inputs[8], sice.at[blocks : 2 * blocks], load_sem.at[8]))
    for each in loads:
        each.start()

    def remote(source, target, sends, receives, number, where):
        return pltpu.make_async_remote_copy(
            src_ref=source, dst_ref=target, send_sem=sends.at[number], recv_sem=receives.at[number],
            device_id=where, device_id_type=MESH,
        )

    down, up = [], []
    for number, (source, stage) in enumerate(zip(inputs, stages)):
        extra = EXTRA if number in (0, 7) else 0
        down.append(remote(
            at_rows(source, slice(0, MARGIN + extra)),
            at_rows(stage, slice(MARGIN + rows, 2 * MARGIN + rows + extra)),
            send_y, recv_y, number, {"gy": lower},
        ))
        up.append(remote(
            at_rows(source, slice(rows - MARGIN, rows)),
            at_rows(stage, slice(0, MARGIN)),
            send_y, recv_y, 9 + number, {"gy": upper},
        ))
    down.append(remote(inputs[8], sice.at[2 * blocks : 3 * blocks], send_y, recv_y, 8, {"gy": lower}))
    up.append(remote(inputs[8], sice.at[0:blocks], send_y, recv_y, 17, {"gy": upper}))

    others = has_lo.astype(jnp.int32) + has_hi.astype(jnp.int32)
    pl.semaphore_wait(barrier, 2 + (ens_count - 1) + 3 * others)

    @pl.when(has_lo)
    def _():
        for each in down:
            each.start()

    @pl.when(has_hi)
    def _():
        for each in up:
            each.start()

    for each in loads:
        each.wait()

    block_cols = sice.shape[1]
    spread = (
        lax.broadcasted_iota(jnp.int32, (block_cols, cols), 1) // BLOCK
        == lax.broadcasted_iota(jnp.int32, (block_cols, cols), 0)
    ).astype(jnp.float32)

    repeat = (
        lax.broadcasted_iota(jnp.int32, (8 * blocks, blocks), 0) // 8
        == lax.broadcasted_iota(jnp.int32, (8 * blocks, blocks), 1)
    ).astype(jnp.float32)

    def expand_ice(part):
        flags = sice[part * blocks : (part + 1) * blocks].astype(jnp.float32)
        flags = jnp.dot(repeat, flags, preferred_element_type=jnp.float32)
        expand[8 * part * blocks : 8 * (part + 1) * blocks] = jnp.dot(
            flags, spread, preferred_element_type=jnp.float32)

    def convert(start, count, ice_row, target):
        at = pl.ds(start, count)
        to = pl.ds(target, count)
        row = lax.broadcasted_iota(jnp.int32, (count, LANES), 0) + (gy * rows + (start - MARGIN))
        coriolis = CORIOLIS_TOP * (row.astype(jnp.float32) + 0.5) / (rows * gy_count)
        for t in range(main):
            c = slice(t * LANES, (t + 1) * LANES)
            present = jnp.concatenate([expand[pl.ds(ice_row, 8), c]] * (count // 8))
            alive = smask[at, c].astype(jnp.float32) * present
            field["u"][t, to] = svel[0, at, c] * alive
            field["v"][t, to] = svel[1, at, c] * alive
            one, two = sstress[0, at, c], sstress[1, at, c]
            field["plus"][t, to] = one + two
            field["minus"][t, to] = one - two
            field["twice"][t, to] = 2.0 * sstress[2, at, c]
            factor = RELAX_RATE * 0.5 / GAIN
            field["pressure"][t, to] = factor * sthick[at, c] * jnp.exp(-STRENGTH_DECAY * (1.0 - sconc[at, c]))
            heavy = smass[at, c]
            heavy = jnp.where(heavy == 0.0, 1.0, heavy)
            turn = coriolis * heavy
            ce, cn = scur[0, at, c], scur[1, at, c]
            field["inertia"][t, to] = heavy / TIME_STEP
            field["turning"][t, to] = turn
            field["bound"][t, to] = jnp.where(alive == 0.0, jnp.inf, turn * turn)
            field["ge"][t, to] = swind[0, at, c] + turn * cn
            field["gn"][t, to] = swind[1, at, c] - turn * ce
            field["ce"][t, to] = ce
            field["cn"][t, to] = cn
            field["cae"][t, to] = alive * ce
            field["can"][t, to] = alive * cn

    expand_ice(1)

    own_at = (PAD + MARGIN, bases[1] + MARGIN)
    for half in range(2):
        def convert_own(block, _, half=half):
            start = pl.multiple_of(half * half_rows + block * BLOCK, 8)
            convert(
                MARGIN + start, BLOCK, pl.multiple_of(8 * (blocks + half * blocks // 2 + block), 8),
                pl.multiple_of(own_at[half] + block * BLOCK, 8),
            )
            return 0

        lax.fori_loop(0, blocks // 2, convert_own, 0)
    convert(MARGIN + half_rows, MARGIN, 8 * (blocks + blocks // 2), own_at[0] + half_rows)
    convert(half_rows, MARGIN, 8 * (blocks + blocks // 2 - 1), bases[1])

    def message(name, tile, at):
        value = field[name][tile, at]
        return jnp.where(field["bound"][tile, at] == jnp.inf, 0.0, value) if name == "inertia" else value

    def packed(fields, at, count):
        lanes = lane_index(count)
        east = jnp.zeros((count, LANES), jnp.float32)
        west = jnp.zeros((count, LANES), jnp.float32)
        for number in fields:
            name, width = PACKED[number]
            start = OFFSETS[number]
            here = jnp.logical_and(lanes >= start, lanes < start + width)
            east = jnp.where(here, rolled(message(name, main - 1, at), start - (LANES - MARGIN)), east)
            west = jnp.where(here, rolled(message(name, 0, at), start), west)
        return east, west

    whole, part = range(WHOLE), range(WHOLE, len(PACKED))

    for half in range(2):
        def pack_own(block, _, half=half):
            start = pl.multiple_of(block * BLOCK, 8)
            east, west = packed(whole, pl.ds(own_at[half] + start, BLOCK), BLOCK)
            to = pl.ds(half * half_rows + start, BLOCK)
            out_a[0, to] = east
            out_a[1, to] = west
            return 0

        lax.fori_loop(0, blocks // 2, pack_own, 0)

    def pack_half(block, _):
        start = pl.multiple_of(block * BLOCK, 8)
        east, west = packed(part, pl.ds(own_at[0] + start, BLOCK), BLOCK)
        more_east, more_west = packed(part, pl.ds(own_at[1] + start, BLOCK), BLOCK)
        second = lane_index(BLOCK) >= HALF
        out_b[0, pl.ds(start, BLOCK)] = jnp.where(second, rolled(more_east, HALF), east)
        out_b[1, pl.ds(start, BLOCK)] = jnp.where(second, rolled(more_west, HALF), west)
        return 0

    lax.fori_loop(0, blocks // 2, pack_half, 0)

    sides = (right, left)
    across, corner_lo, corner_hi = [], [], []
    for side, to in enumerate(sides):
        across.append(remote(
            out_a.at[side], in_a.at[side, MARGIN : MARGIN + rows], send_x, recv_x, 2 * side, {"gx": to}))
        across.append(remote(
            out_b.at[side], in_b.at[side, MARGIN : MARGIN + half_rows], send_x, recv_x, 2 * side + 1, {"gx": to}))
        lo, hi = {"gx": to, "gy": lower}, {"gx": to, "gy": upper}
        corner_lo.append(remote(
            out_a.at[side, 0 : MARGIN + EXTRA],
            in_a.at[side, MARGIN + rows : 2 * MARGIN + rows + EXTRA],
            send_d, recv_d, 4 * side, lo))
        corner_lo.append(remote(
            out_b.at[side, 0:MARGIN],
            in_b.at[side, MARGIN + half_rows : 2 * MARGIN + half_rows],
            send_d, recv_d, 4 * side + 1, lo))
        corner_hi.append(remote(
            out_a.at[side, rows - MARGIN : rows], in_a.at[side, 0:MARGIN],
            send_d, recv_d, 4 * side + 2, hi))
        corner_hi.append(remote(
            out_b.at[side, half_rows - MARGIN : half_rows], in_b.at[side, 0:MARGIN],
            send_d, recv_d, 4 * side + 3, hi))
    for each in across:
        each.start()

    @pl.when(has_lo)
    def _():
        for each in corner_lo:
            each.start()

    @pl.when(has_hi)
    def _():
        for each in corner_hi:
            each.start()

    def strip_columns(target, count):
        at = pl.ds(target, count)
        lanes = lane_index(count)
        for name, _ in PACKED:
            field[name][main, at] = jnp.where(
                lanes < OWN, message(name, 0, at), rolled(message(name, main - 1, at), AT_HALO - LANES))

    for half in range(2):
        def own_columns(block, _, half=half):
            strip_columns(pl.multiple_of(own_at[half] + block * BLOCK, 8), BLOCK)
            return 0

        lax.fori_loop(0, blocks // 2, own_columns, 0)
    strip_columns(own_at[0] + half_rows, MARGIN)
    strip_columns(bases[1], MARGIN)

    @pl.when(has_lo)
    def _():
        for each in up:
            each.wait_recv()

    @pl.when(jnp.logical_not(has_lo))
    def _():
        for stage in stages:
            for index in range(stage.shape[0]) if len(stage.shape) == 3 else (None,):
                view = stage if index is None else stage.at[index]
                view[0:MARGIN] = jnp.zeros((MARGIN, cols), stage.dtype)
        sice[0:blocks] = jnp.zeros((blocks, block_cols), jnp.int32)

    @pl.when(has_hi)
    def _():
        for each in down:
            each.wait_recv()

    @pl.when(jnp.logical_not(has_hi))
    def _():
        for stage in stages:
            count = stage.shape[-2] - MARGIN - rows
            for index in range(stage.shape[0]) if len(stage.shape) == 3 else (None,):
                view = stage if index is None else stage.at[index]
                view[MARGIN + rows : MARGIN + rows + count] = jnp.zeros((count, cols), stage.dtype)
        sice[2 * blocks : 3 * blocks] = jnp.zeros((blocks, block_cols), jnp.int32)

    expand_ice(0)
    expand_ice(2)
    convert(0, MARGIN, 8 * (blocks - 1), bases[0])
    convert(MARGIN + rows, MARGIN, 16 * blocks, own_at[1] + half_rows)
    beyond = slice(2 * MARGIN + rows, 2 * MARGIN + rows + EXTRA)
    past = slice(bases[1] + reach, bases[1] + reach + EXTRA)
    other_past = slice(bases[0] + reach, bases[0] + reach + EXTRA)
    for t in range(main):
        c = slice(t * LANES, (t + 1) * LANES)
        alive = smask[beyond, c].astype(jnp.float32) * expand[16 * blocks : 16 * blocks + 8, c]
        field["u"][t, past] = svel[0, beyond, c] * alive
        field["v"][t, past] = svel[1, beyond, c] * alive

    for each in across:
        each.wait_recv()

    @pl.when(has_lo)
    def _():
        for each in corner_hi:
            each.wait_recv()

    @pl.when(jnp.logical_not(has_lo))
    def _():
        for side in range(2):
            in_a[side, 0:MARGIN] = jnp.zeros((MARGIN, LANES), jnp.float32)
            in_b[side, 0:MARGIN] = jnp.zeros((MARGIN, LANES), jnp.float32)

    @pl.when(has_hi)
    def _():
        for each in corner_lo:
            each.wait_recv()

    @pl.when(jnp.logical_not(has_hi))
    def _():
        for side in range(2):
            in_a[side, MARGIN + rows :] = jnp.zeros((MARGIN + EXTRA, LANES), jnp.float32)
            in_b[side, MARGIN + half_rows :] = jnp.zeros((MARGIN, LANES), jnp.float32)

    def strip_value(number, row, target, count, half_start, half_lane):
        name, width = PACKED[number]
        lanes = lane_index(count)
        if number < WHOLE:
            arrived, there, lane = in_a, pl.ds(row + MARGIN, count), OFFSETS[number]
        else:
            arrived, there, lane = in_b, pl.ds(half_start, count), OFFSETS[number] + half_lane
        value = jnp.where(lanes < AT_HALO + width, rolled(arrived[1, there], AT_HALO - lane), 0.0)
        value = jnp.where(lanes < AT_HALO, field[name][main, pl.ds(target, count)], value)
        return jnp.where(lanes >= AT_LEFT, rolled(arrived[0, there], AT_LEFT - lane), value)

    def strip_rows(first, target, count, half_start, half_lane):
        at = pl.ds(target, count)
        value = {
            name: strip_value(number, first, target, count, half_start, half_lane)
            for number, (name, _) in enumerate(PACKED)
        }
        row = lax.broadcasted_iota(jnp.int32, (count, LANES), 0) + (gy * rows + first)
        coriolis = CORIOLIS_TOP * (row.astype(jnp.float32) + 0.5) / (rows * gy_count)
        empty = value["inertia"] == 0.0
        alive = jnp.where(empty, 0.0, 1.0)
        heavy = jnp.where(empty, 1.0 / TIME_STEP, value["inertia"])
        value["inertia"] = heavy
        value["turning"] = coriolis * (heavy * TIME_STEP)
        value["bound"] = jnp.where(empty, jnp.inf, value["turning"] * value["turning"])
        value["cae"] = alive * value["ce"]
        value["can"] = alive * value["cn"]
        for name, each in value.items():
            field[name][main, at] = each

    for half in range(2):
        def strip_own(block, _, half=half):
            start = pl.multiple_of(block * BLOCK, 8)
            strip_rows(half * half_rows + start, pl.multiple_of(own_at[half] + start, 8), BLOCK,
                       MARGIN + start, half * HALF)
            return 0

        lax.fori_loop(0, blocks // 2, strip_own, 0)
    strip_rows(half_rows, own_at[0] + half_rows, MARGIN, MARGIN, HALF)
    strip_rows(half_rows - MARGIN, bases[1], MARGIN, half_rows, 0)
    strip_columns(bases[0], MARGIN)
    strip_columns(own_at[1] + half_rows, MARGIN)
    strip_rows(-MARGIN, bases[0], MARGIN, 0, HALF)
    strip_rows(rows, own_at[1] + half_rows, MARGIN, MARGIN + half_rows, 0)
    for number in range(2):
        name = PACKED[number][0]
        lanes = lane_index(EXTRA)
        field[name][main, past] = jnp.where(
            lanes < OWN, field[name][0, past], rolled(field[name][main - 1, past], AT_HALO - LANES))
        field[name][main, past] = strip_value(number, rows + MARGIN, past.start, EXTRA, 0, 0)
        for t in range(tiles):
            field[name][t, other_past] = field[name][t, bases[1] + 2 * MARGIN : bases[1] + 2 * MARGIN + EXTRA]
    for name in ("plus", "minus", "twice"):
        for t in range(tiles):
            for base in bases:
                field[name][t, base - PAD : base] = jnp.zeros((PAD, LANES), jnp.float32)

    u, v, plus, minus, twice = (field[name] for name in ("u", "v", "plus", "minus", "twice"))
    def ahead(values):
        turned = [rolled(value, -1) for value in values]
        at_end = lane_index(values[0].shape[0]) == LANES - 1
        return [jnp.where(at_end, turned[(t + 1) % main], turned[t]) for t in range(main)] + turned[main:]

    def behind(values):
        turned = [rolled(value, 1) for value in values]
        at_start = lane_index(values[0].shape[0]) == 0
        return [jnp.where(at_start, turned[t - 1 if t else main - 1], turned[t]) for t in range(main)] + turned[main:]

    def gradients(start, count):
        add, sub, add_s, sub_s = [], [], [], []
        at, after = pl.ds(start, count), pl.ds(start + 1, count)
        for t in range(tiles):
            u0, u1, v0, v1 = u[t, at], u[t, after], v[t, at], v[t, after]
            a, b, c, d = u0 + u1, u1 - u0, v0 + v1, v1 - v0
            add.append(a + d)
            sub.append(a - d)
            add_s.append(b + c)
            sub_s.append(b - c)
        return add, sub, add_s, sub_s

    def stress_sums(start):
        at, before = pl.ds(start, STEP), pl.ds(start - 1, STEP)
        e_near, e_far, n_near, n_far = [], [], [], []
        for t in range(tiles):
            p1, p0 = plus[t, at], plus[t, before]
            m1, m0 = minus[t, at], minus[t, before]
            s1, s0 = twice[t, at], twice[t, before]
            a, d, b, e = p0 + p1, s1 - s0, s0 + s1, m1 - m0
            e_near.append(a + d)
            e_far.append(a - d)
            n_near.append(b + e)
            n_far.append(b - e)
        return e_near, e_far, n_near, n_far

    def stress_rows(start, growth):
        at = pl.ds(start, STEP)
        for t in range(tiles):
            div = field["add_next"][t, at] - field["sub"][t, at]
            tension = field["sub_next"][t, at] - field["add"][t, at]
            shear = field["shear_next"][t, at] + field["sub_s"][t, at]
            square = div * div + (1.0 / ECCENTRICITY_SQUARED) * (tension * tension + shear * shear)
            inverse = lax.rsqrt(jnp.maximum(square, TINY))
            weight = (field["pressure"][t, at] * growth) * jnp.minimum(inverse, 1.0)
            quarter = weight * (1.0 / ECCENTRICITY_SQUARED)
            change = weight * (div - square * inverse)
            other = quarter * tension
            plus[t, at] = plus[t, at] + (change + other)
            minus[t, at] = minus[t, at] + (change - other)
            twice[t, at] = twice[t, at] + quarter * shear

    def velocity_rows(start, scale):
        at = pl.ds(start, STEP)
        for t in range(tiles):
            de, dn = u[t, at] - field["ce"][t, at], v[t, at] - field["cn"][t, at]
            square = de * de + dn * dn
            drag = square * lax.rsqrt(jnp.maximum(square, TINY))
            heavy, turn = field["inertia"][t, at], field["turning"][t, at]
            diag = heavy + drag
            force_e = (field["e_near"][t, at] - field["e_back"][t, at]) * scale
            force_n = (field["n_near"][t, at] - field["n_back"][t, at]) * scale
            push_e = heavy * de + (force_e + field["ge"][t, at])
            push_n = heavy * dn + (force_n + field["gn"][t, at])
            inverse = lax.rsqrt(diag * diag + field["bound"][t, at])
            inverse = inverse * inverse
            u[t, at] = (diag * push_e + turn * push_n) * inverse + field["cae"][t, at]
            v[t, at] = (diag * push_n - turn * push_e) * inverse + field["can"][t, at]

    def advance(base):
        last = base + reach - STEP

        def step(_, carried):
            at_g, at_s, at_f, at_v, growth, growth_s, scale, scale_s, scale_f, scale_v = carried
            at_g, at_s, at_f, at_v = (pl.multiple_of(each, 8) for each in (at_g, at_s, at_f, at_v))

            def keep(names, values, start):
                for name, each in zip(names, values):
                    for t in range(tiles):
                        field[name][t, pl.ds(start, STEP)] = each[t]

            add, sub, add_s, sub_s = gradients(at_g, STEP)
            add_next, sub_next, shear_next = ahead(add), ahead(sub), ahead(add_s)
            e_near, e_far, n_near, n_far = stress_sums(at_f)
            e_back, n_back = behind(e_far), behind(n_far)
            stress_rows(at_s, growth_s)
            velocity_rows(at_v, scale_v)
            keep(("add", "sub", "sub_s", "add_next", "sub_next", "shear_next"),
                 (add, sub, sub_s, add_next, sub_next, shear_next), at_g)
            keep(("e_near", "n_near", "e_back", "n_back"), (e_near, n_near, e_back, n_back), at_f)
            wrap = at_g == last
            return (
                jnp.where(wrap, base, jnp.where(at_g == spare, spare, at_g + STEP)), at_g, at_s, at_f,
                jnp.where(wrap, growth * GAIN, growth), growth,
                jnp.where(wrap, scale * (1.0 / GAIN), scale), scale, scale_s, scale_f,
            )

        one = jnp.float32(1.0)
        empty = jnp.int32(spare)
        start = (jnp.int32(base), empty, empty, empty, one * GAIN, one, one * (0.25 / GAIN), one, one, one)
        carried = lax.fori_loop(0, SUBCYCLES * (reach // STEP), step, start)
        lax.fori_loop(0, 3, step, (empty,) + carried[1:])

    shrink = 0.5 * GAIN**-SUBCYCLES

    def merged(values):
        lanes = lane_index(values[0].shape[0])
        on_left, on_right = lanes < MARGIN, lanes >= LANES - MARGIN - 2
        values = list(values)
        values[0] = jnp.where(on_left, values[main], values[0])
        values[main - 1] = jnp.where(on_right, rolled(values[main], LANES - AT_HALO), values[main - 1])
        return values[:main]

    def finish_conc(start, row, count):
        add, sub, _, _ = gradients(start, count)
        add_next = ahead(add)
        div = merged([add_next[t] - sub[t] for t in range(tiles)])
        for t in range(main):
            c = slice(t * LANES, (t + 1) * LANES)
            value = sconc[pl.ds(MARGIN + row, count), c]
            conc_out[pl.ds(row, count), c] = jnp.clip(value - value * (0.5 * div[t]), 0.0, 1.0)

    def finish(start, row, count):
        here, at = pl.ds(start, count), pl.ds(row, count)
        east, north, one, two, three = (
            merged([ref[t, here] for t in range(tiles)]) for ref in (u, v, plus, minus, twice)
        )
        for t in range(main):
            c = slice(t * LANES, (t + 1) * LANES)
            vel_out[0, at, c] = east[t]
            vel_out[1, at, c] = north[t]
            stress_out[0, at, c] = (one[t] + two[t]) * shrink
            stress_out[1, at, c] = (one[t] - two[t]) * shrink
            stress_out[2, at, c] = three[t] * shrink
        finish_conc(start, row, count)

    def finish_half(half):
        def body(block, _):
            start = block * BLOCK
            finish(
                pl.multiple_of(jnp.where(half == 0, own_at[0], own_at[1]) + start, 8),
                pl.multiple_of(half * half_rows + start, 8), BLOCK,
            )
            return 0

        lax.fori_loop(0, half_rows // BLOCK, body, 0)

    early = (1 - me) if ens_count == 2 else jnp.int32(0)
    late = 1 - early
    share = rows // ens_count
    swaps = []
    for step, peer in enumerate(peers):
        part_of = pl.ds(pl.multiple_of(peer * share, 8), share)
        swaps.append(remote(
            vel_out.at[:, part_of], landing.at[step, 1:3], send_e, recv_e, 2 * step, {"ens": peer}))
        swaps.append(remote(
            conc_out.at[part_of], landing.at[step, 0], send_e, recv_e, 2 * step + 1, {"ens": peer}))

    advance(jnp.where(early == 0, bases[0], bases[1]))
    finish_half(early)
    if ens_count == 2:
        for each in swaps:
            each.start()
    advance(jnp.where(late == 0, bases[0], bases[1]))
    finish_half(late)
    if ens_count != 2:
        for each in swaps:
            each.start()
    for each in across:
        each.wait_send()

    @pl.when(has_lo)
    def _():
        for each in down + corner_lo:
            each.wait_send()

    @pl.when(has_hi)
    def _():
        for each in up + corner_hi:
            each.wait_send()

    for each in swaps:
        each.wait_recv()
    for each in swaps:
        each.wait_send()


def write_kernel(count, vel, stress, conc, landing, vel_out, stress_out, mean_out, spread_out, mean, spread, sems):
    copies = [
        pltpu.make_async_copy(vel, vel_out, sems.at[0]),
        pltpu.make_async_copy(stress, stress_out, sems.at[1]),
    ]
    for each in copies:
        each.start()
    share = mean.shape[1]
    own = pl.ds(pl.multiple_of(lax.axis_index("ens") * share, 8), share)
    for f in range(3):
        values = [conc[own] if f == 0 else vel[f - 1, own]]
        values += [landing[step, f] for step in range(count - 1)]
        average = functools.reduce(jnp.add, values) / count
        mean[f] = average
        spread[f] = functools.reduce(jnp.add, [(v - average) * (v - average) for v in values]) / count
    more = [
        pltpu.make_async_copy(mean, mean_out, sems.at[2]),
        pltpu.make_async_copy(spread, spread_out, sems.at[3]),
    ]
    for each in more:
        each.start()
    for each in copies + more:
        each.wait()


def solution(mesh):
    gx_count, gy_count, ens_count = mesh.shape["gx"], mesh.shape["gy"], mesh.shape["ens"]
    f32 = jnp.float32

    def vmem(*shape, dtype=f32):
        return pltpu.VMEM(shape, dtype)

    def specs(count, space):
        return [pl.BlockSpec(memory_space=space)] * count

    def body(velocity, stress, thickness, concentration, node_mass, wind, current, mask, ice):
        rows, cols = mask.shape
        share = rows // ens_count
        tiles = cols // LANES + 1
        block_rows, block_cols = ice.shape[1:]
        tall = rows + 2 * MARGIN
        total = -(-(5 * PAD + 2 * (rows // 2 + 2 * MARGIN) + STEP + PAD) // 32) * 32
        shape = lambda *dims: jax.ShapeDtypeStruct(dims, f32)
        dma = lambda count: pltpu.SemaphoreType.DMA((count,))
        state = pl.pallas_call(
            functools.partial(step_kernel, (gx_count, gy_count, ens_count)),
            name="subcycles",
            out_shape=(
                shape(2, rows, cols),
                shape(3, rows, cols),
                shape(rows, cols),
                shape(ens_count - 1, 3, share, cols),
            ),
            in_specs=specs(9, pltpu.HBM),
            out_specs=tuple(specs(4, pltpu.VMEM)),
            scratch_shapes=[vmem(tiles, total, LANES)] * len(MAIN_FIELDS)
            + [
                vmem(2, tall + EXTRA, cols),
                vmem(3, tall, cols),
                vmem(tall, cols),
                vmem(tall, cols),
                vmem(tall, cols),
                vmem(2, tall, cols),
                vmem(2, tall, cols),
                vmem(tall + EXTRA, cols, dtype=jnp.int32),
                vmem(3 * block_rows, block_cols, dtype=jnp.int32),
                vmem(24 * block_rows, cols),
                vmem(2, rows, LANES),
                vmem(2, rows // 2, LANES),
                vmem(2, tall + EXTRA, LANES),
                vmem(2, rows // 2 + 2 * MARGIN, LANES),
                dma(9), dma(18), dma(18), dma(4), dma(4), dma(8), dma(8),
                dma(2 * (ens_count - 1)), dma(2 * (ens_count - 1)),
            ],
            compiler_params=pltpu.CompilerParams(
                collective_id=0, has_side_effects=True, vmem_limit_bytes=28 << 20),
        )(*(pltpu.with_memory_space_constraint(each, pltpu.HBM) for each in (
            velocity[0], stress[0], thickness[0], concentration[0], node_mass[0], wind[0], current[0], mask, ice[0])))
        vel_out, stress_out, mean, spread = pl.pallas_call(
            functools.partial(write_kernel, ens_count),
            name="write",
            out_shape=(shape(2, rows, cols), shape(3, rows, cols), shape(3, share, cols), shape(3, share, cols)),
            in_specs=specs(4, pltpu.VMEM),
            out_specs=tuple(specs(4, pltpu.HBM)),
            scratch_shapes=[vmem(3, share, cols), vmem(3, share, cols), dma(4)],
            compiler_params=pltpu.CompilerParams(vmem_limit_bytes=4 << 20),
        )(*state)
        return vel_out[None], stress_out[None], mean, spread

    grid = P("ens", "gy", "gx")
    pair = P("ens", None, "gy", "gx")
    split = P(None, ("gy", "ens"), "gx")
    return jax.shard_map(
        body,
        mesh=mesh,
        in_specs=(pair, pair, grid, grid, grid, pair, pair, P("gy", "gx"), grid),
        out_specs=(pair, pair, split, split),
        check_vma=False,
    )
```

```python
import functools

import jax
import jax.numpy as jnp
from jax import lax
from jax.experimental import pallas as pl
from jax.experimental.pallas import tpu as pltpu
from jax.sharding import PartitionSpec as P

SUBCYCLES = 16
BLOCK = 32

TIME_STEP = 0.5
RELAX_RATE = 0.25
ECCENTRICITY_SQUARED = 4.0
CORIOLIS_TOP = 1.0
STRENGTH_DECAY = 20.0

MESH = pl.DeviceIdType.MESH
LANES = 128
TINY = 1.1754944e-38
GAIN = 1.0 + RELAX_RATE

MARGIN = SUBCYCLES
EXTRA = 8
PAD = 8
CHUNK = 64
STEP = 32

PACKED = (
    ("u", MARGIN + 1), ("v", MARGIN + 1), ("plus", MARGIN), ("minus", MARGIN), ("twice", MARGIN),
    ("pressure", MARGIN), ("inertia", MARGIN),
    ("ge", MARGIN), ("gn", MARGIN), ("ce", MARGIN), ("cn", MARGIN),
)
WHOLE = 7
OFFSETS = []
for _i, (_, _w) in enumerate(PACKED):
    if _i == 0 or _i == WHOLE:
        OFFSETS.append(0)
    else:
        OFFSETS.append(OFFSETS[-1] + PACKED[_i - 1][1])
HALF = LANES // 2

OWN = 36
AT_RIGHT = 48
AT_HALO = AT_RIGHT + OWN
AT_LEFT = LANES - MARGIN

MAIN_FIELDS = (
    "u", "v", "plus", "minus", "twice", "pressure", "inertia", "turning",
    "ge", "gn", "ce", "cn", "bound",
    "u_next", "v_next", "e_near", "n_near", "e_back", "n_back",
)


def lane_index(rows):
    return lax.broadcasted_iota(jnp.int32, (rows, LANES), 1)


def rolled(value, shift):
    shift = shift % LANES
    return value if shift == 0 else pltpu.roll(value, shift, 1)


def step_kernel(sizes, *refs):
    gx_count, gy_count, ens_count = sizes
    inputs, refs = refs[:9], refs[9:]
    (vel_out, stress_out, conc_out, landing), refs = refs[:4], refs[4:]
    arrays, refs = refs[: len(MAIN_FIELDS)], refs[len(MAIN_FIELDS) :]
    (svel, sstress, sthick, sconc, smass, swind, scur, smask, sice, expand), refs = refs[:10], refs[10:]
    (out_a, out_b, in_a, in_b, load_sem, send_y, recv_y, send_x, recv_x, send_d, recv_d, send_e, recv_e) = refs
    field = dict(zip(MAIN_FIELDS, arrays))
    stages = (svel, sstress, sthick, sconc, smass, swind, scur, smask)
    rows, cols = conc_out.shape
    main = cols // LANES
    tiles = main + 1
    blocks = rows // BLOCK
    half_rows = rows // 2
    reach = half_rows + 2 * MARGIN
    bases = (PAD, 3 * PAD + reach)
    first_rows = (-MARGIN, half_rows - MARGIN)
    spare = 5 * PAD + 2 * reach
    gx, gy, me = lax.axis_index("gx"), lax.axis_index("gy"), lax.axis_index("ens")
    right, left = lax.rem(gx + 1, gx_count), lax.rem(gx + gx_count - 1, gx_count)
    has_lo, has_hi = gy > 0, gy < gy_count - 1
    lower, upper = jnp.maximum(gy - 1, 0), jnp.minimum(gy + 1, gy_count - 1)
    peers = [lax.rem(me + step, ens_count) for step in range(1, ens_count)]

    barrier = pltpu.get_barrier_semaphore()

    def greet(**where):
        pl.semaphore_signal(barrier, inc=1, device_id=where, device_id_type=MESH)

    greet(gx=left)
    greet(gx=right)
    for peer in peers:
        greet(ens=peer)
    for there, row in ((has_lo, lower), (has_hi, upper)):
        @pl.when(there)
        def _(row=row):
            greet(gy=row)
            greet(gy=row, gx=left)
            greet(gy=row, gx=right)

    def at_rows(ref, where):
        return ref.at[:, where] if len(ref.shape) == 3 else ref.at[where]

    loads = [[
        pltpu.make_async_copy(
            at_rows(source, slice(half * half_rows, (half + 1) * half_rows)),
            at_rows(stage, slice(MARGIN + half * half_rows, MARGIN + (half + 1) * half_rows)),
            load_sem.at[8 * half + number],
        )
        for number, (source, stage) in enumerate(zip(inputs, stages))
    ] for half in range(2)]
    loads[0].append(pltpu.make_async_copy(inputs[8], sice.at[blocks : 2 * blocks], load_sem.at[16]))
    for each in loads[0] + loads[1]:
        each.start()

    def remote(source, target, sends, receives, number, where):
        return pltpu.make_async_remote_copy(
            src_ref=source, dst_ref=target, send_sem=sends.at[number], recv_sem=receives.at[number],
            device_id=where, device_id_type=MESH,
        )

    down, up = [], []
    for number, (source, stage) in enumerate(zip(inputs, stages)):
        extra = EXTRA if number in (0, 7) else 0
        down.append(remote(
            at_rows(source, slice(0, MARGIN + extra)),
            at_rows(stage, slice(MARGIN + rows, 2 * MARGIN + rows + extra)),
            send_y, recv_y, number, {"gy": lower},
        ))
        up.append(remote(
            at_rows(source, slice(rows - MARGIN, rows)),
            at_rows(stage, slice(0, MARGIN)),
            send_y, recv_y, 9 + number, {"gy": upper},
        ))
    down.append(remote(inputs[8], sice.at[2 * blocks : 3 * blocks], send_y, recv_y, 8, {"gy": lower}))
    up.append(remote(inputs[8], sice.at[0:blocks], send_y, recv_y, 17, {"gy": upper}))

    others = has_lo.astype(jnp.int32) + has_hi.astype(jnp.int32)
    pl.semaphore_wait(barrier, 2 + (ens_count - 1) + 3 * others)

    @pl.when(has_lo)
    def _():
        for each in down:
            each.start()

    @pl.when(has_hi)
    def _():
        for each in up:
            each.start()

    block_cols = sice.shape[1]
    spread = (
        lax.broadcasted_iota(jnp.int32, (block_cols, cols), 1) // BLOCK
        == lax.broadcasted_iota(jnp.int32, (block_cols, cols), 0)
    ).astype(jnp.float32)

    repeat = (
        lax.broadcasted_iota(jnp.int32, (8 * blocks, blocks), 0) // 8
        == lax.broadcasted_iota(jnp.int32, (8 * blocks, blocks), 1)
    ).astype(jnp.float32)

    def expand_ice(part):
        flags = sice[part * blocks : (part + 1) * blocks].astype(jnp.float32)
        flags = jnp.dot(repeat, flags, preferred_element_type=jnp.float32)
        expand[8 * part * blocks : 8 * (part + 1) * blocks] = jnp.dot(
            flags, spread, preferred_element_type=jnp.float32)

    def convert(start, count, ice_row, target):
        at = pl.ds(start, count)
        to = pl.ds(target, count)
        row = lax.broadcasted_iota(jnp.int32, (count, LANES), 0) + (gy * rows + (start - MARGIN))
        coriolis = CORIOLIS_TOP * (row.astype(jnp.float32) + 0.5) / (rows * gy_count)
        sent = []
        for t in range(main):
            c = slice(t * LANES, (t + 1) * LANES)
            present = jnp.concatenate([expand[pl.ds(ice_row, 8), c]] * (count // 8))
            alive = smask[at, c].astype(jnp.float32) * present
            one, two = sstress[0, at, c], sstress[1, at, c]
            factor = RELAX_RATE * 0.5 / GAIN
            heavy = smass[at, c]
            heavy = jnp.where(heavy == 0.0, 1.0, heavy)
            turn = coriolis * heavy
            ce, cn = scur[0, at, c], scur[1, at, c]
            value = {
                "u": svel[0, at, c] * alive,
                "v": svel[1, at, c] * alive,
                "plus": one + two,
                "minus": one - two,
                "twice": 2.0 * sstress[2, at, c],
                "pressure": factor * sthick[at, c] * jnp.exp(-STRENGTH_DECAY * (1.0 - sconc[at, c])),
                "inertia": heavy / TIME_STEP,
                "turning": turn,
                "bound": jnp.where(alive == 0.0, jnp.inf, turn * turn),
                "ge": swind[0, at, c] + turn * cn,
                "gn": swind[1, at, c] - turn * ce,
                "ce": alive * ce,
                "cn": alive * cn,
            }
            for name, each in value.items():
                field[name][t, to] = each
            value["inertia"] = value["inertia"] * alive
            sent.append(value)
        return sent

    whole, part = range(WHOLE), range(WHOLE, len(PACKED))

    def packed(sent, fields, shift, east, west):
        lanes = lane_index(east.shape[0])
        for number in fields:
            name, width = PACKED[number]
            start = OFFSETS[number] + shift
            here = jnp.logical_and(lanes >= start, lanes < start + width)
            east = jnp.where(here, rolled(sent[main - 1][name], start - (LANES - MARGIN)), east)
            west = jnp.where(here, rolled(sent[0][name], start), west)
        return east, west

    own_at = (PAD + MARGIN, bases[1] + MARGIN)
    for half in range(2):
        for each in loads[half]:
            each.wait()
        if half == 0:
            expand_ice(1)

        def convert_own(block, _, half=half):
            start = pl.multiple_of(half * half_rows + block * BLOCK, 8)
            sent = convert(
                MARGIN + start, BLOCK, pl.multiple_of(8 * (blocks + half * blocks // 2 + block), 8),
                pl.multiple_of(own_at[half] + block * BLOCK, 8),
            )
            zero = jnp.zeros((BLOCK, LANES), jnp.float32)
            to, to_half = pl.ds(start, BLOCK), pl.ds(pl.multiple_of(block * BLOCK, 8), BLOCK)
            out_a[0, to], out_a[1, to] = packed(sent, whole, 0, zero, zero)
            before = (out_b[0, to_half], out_b[1, to_half]) if half else (zero, zero)
            out_b[0, to_half], out_b[1, to_half] = packed(sent, part, half * HALF, *before)
            return 0

        lax.fori_loop(0, blocks // 2, convert_own, 0)

    def message(name, tile, at):
        value = field[name][tile, at]
        return jnp.where(field["bound"][tile, at] == jnp.inf, 0.0, value) if name == "inertia" else value

    sides = (right, left)
    across, corner_lo, corner_hi = [], [], []
    for side, to in enumerate(sides):
        across.append(remote(
            out_a.at[side], in_a.at[side, MARGIN : MARGIN + rows], send_x, recv_x, 2 * side, {"gx": to}))
        across.append(remote(
            out_b.at[side], in_b.at[side, MARGIN : MARGIN + half_rows], send_x, recv_x, 2 * side + 1, {"gx": to}))
        lo, hi = {"gx": to, "gy": lower}, {"gx": to, "gy": upper}
        corner_lo.append(remote(
            out_a.at[side, 0 : MARGIN + EXTRA],
            in_a.at[side, MARGIN + rows : 2 * MARGIN + rows + EXTRA],
            send_d, recv_d, 4 * side, lo))
        corner_lo.append(remote(
            out_b.at[side, 0:MARGIN],
            in_b.at[side, MARGIN + half_rows : 2 * MARGIN + half_rows],
            send_d, recv_d, 4 * side + 1, lo))
        corner_hi.append(remote(
            out_a.at[side, rows - MARGIN : rows], in_a.at[side, 0:MARGIN],
            send_d, recv_d, 4 * side + 2, hi))
        corner_hi.append(remote(
            out_b.at[side, half_rows - MARGIN : half_rows], in_b.at[side, 0:MARGIN],
            send_d, recv_d, 4 * side + 3, hi))
    for each in across:
        each.start()

    @pl.when(has_lo)
    def _():
        for each in corner_lo:
            each.start()

    @pl.when(has_hi)
    def _():
        for each in corner_hi:
            each.start()

    convert(MARGIN + half_rows, MARGIN, 8 * (blocks + blocks // 2), own_at[0] + half_rows)
    convert(half_rows, MARGIN, 8 * (blocks + blocks // 2 - 1), bases[1])

    def strip_columns(target, count):
        at = pl.ds(target, count)
        lanes = lane_index(count)
        for name, _ in PACKED:
            field[name][main, at] = jnp.where(
                lanes < OWN, message(name, 0, at), rolled(message(name, main - 1, at), AT_HALO - LANES))

    for half in range(2):
        def own_columns(block, _, half=half):
            strip_columns(pl.multiple_of(own_at[half] + block * CHUNK, 8), CHUNK)
            return 0

        lax.fori_loop(0, half_rows // CHUNK, own_columns, 0)
    strip_columns(own_at[0] + half_rows, MARGIN)
    strip_columns(bases[1], MARGIN)

    @pl.when(has_lo)
    def _():
        for each in up:
            each.wait_recv()

    @pl.when(jnp.logical_not(has_lo))
    def _():
        for stage in stages:
            for index in range(stage.shape[0]) if len(stage.shape) == 3 else (None,):
                view = stage if index is None else stage.at[index]
                view[0:MARGIN] = jnp.zeros((MARGIN, cols), stage.dtype)
        sice[0:blocks] = jnp.zeros((blocks, block_cols), jnp.int32)

    @pl.when(has_hi)
    def _():
        for each in down:
            each.wait_recv()

    @pl.when(jnp.logical_not(has_hi))
    def _():
        for stage in stages:
            count = stage.shape[-2] - MARGIN - rows
            for index in range(stage.shape[0]) if len(stage.shape) == 3 else (None,):
                view = stage if index is None else stage.at[index]
                view[MARGIN + rows : MARGIN + rows + count] = jnp.zeros((count, cols), stage.dtype)
        sice[2 * blocks : 3 * blocks] = jnp.zeros((blocks, block_cols), jnp.int32)

    expand_ice(0)
    expand_ice(2)
    convert(0, MARGIN, 8 * (blocks - 1), bases[0])
    convert(MARGIN + rows, MARGIN, 16 * blocks, own_at[1] + half_rows)
    beyond = slice(2 * MARGIN + rows, 2 * MARGIN + rows + EXTRA)
    past = slice(bases[1] + reach, bases[1] + reach + EXTRA)
    other_past = slice(bases[0] + reach, bases[0] + reach + EXTRA)
    for t in range(main):
        c = slice(t * LANES, (t + 1) * LANES)
        alive = smask[beyond, c].astype(jnp.float32) * expand[16 * blocks : 16 * blocks + 8, c]
        field["u"][t, past] = svel[0, beyond, c] * alive
        field["v"][t, past] = svel[1, beyond, c] * alive

    for each in across:
        each.wait_recv()

    @pl.when(has_lo)
    def _():
        for each in corner_hi:
            each.wait_recv()

    @pl.when(jnp.logical_not(has_lo))
    def _():
        for side in range(2):
            in_a[side, 0:MARGIN] = jnp.zeros((MARGIN, LANES), jnp.float32)
            in_b[side, 0:MARGIN] = jnp.zeros((MARGIN, LANES), jnp.float32)

    @pl.when(has_hi)
    def _():
        for each in corner_lo:
            each.wait_recv()

    @pl.when(jnp.logical_not(has_hi))
    def _():
        for side in range(2):
            in_a[side, MARGIN + rows :] = jnp.zeros((MARGIN + EXTRA, LANES), jnp.float32)
            in_b[side, MARGIN + half_rows :] = jnp.zeros((MARGIN, LANES), jnp.float32)

    def strip_value(number, row, target, count, half_start, half_lane):
        name, width = PACKED[number]
        lanes = lane_index(count)
        if number < WHOLE:
            arrived, there, lane = in_a, pl.ds(row + MARGIN, count), OFFSETS[number]
        else:
            arrived, there, lane = in_b, pl.ds(half_start, count), OFFSETS[number] + half_lane
        value = jnp.where(lanes < AT_HALO + width, rolled(arrived[1, there], AT_HALO - lane), 0.0)
        value = jnp.where(lanes < AT_HALO, field[name][main, pl.ds(target, count)], value)
        return jnp.where(lanes >= AT_LEFT, rolled(arrived[0, there], AT_LEFT - lane), value)

    def strip_rows(first, target, count, half_start, half_lane):
        at = pl.ds(target, count)
        value = {
            name: strip_value(number, first, target, count, half_start, half_lane)
            for number, (name, _) in enumerate(PACKED)
        }
        row = lax.broadcasted_iota(jnp.int32, (count, LANES), 0) + (gy * rows + first)
        coriolis = CORIOLIS_TOP * (row.astype(jnp.float32) + 0.5) / (rows * gy_count)
        empty = value["inertia"] == 0.0
        heavy = jnp.where(empty, 1.0 / TIME_STEP, value["inertia"])
        value["inertia"] = heavy
        value["turning"] = coriolis * (heavy * TIME_STEP)
        value["bound"] = jnp.where(empty, jnp.inf, value["turning"] * value["turning"])
        for name, each in value.items():
            field[name][main, at] = each

    for half in range(2):
        def strip_own(block, _, half=half):
            start = pl.multiple_of(block * CHUNK, 8)
            strip_rows(half * half_rows + start, pl.multiple_of(own_at[half] + start, 8), CHUNK,
                       MARGIN + start, half * HALF)
            return 0

        lax.fori_loop(0, half_rows // CHUNK, strip_own, 0)
    strip_rows(half_rows, own_at[0] + half_rows, MARGIN, MARGIN, HALF)
    strip_rows(half_rows - MARGIN, bases[1], MARGIN, half_rows, 0)
    strip_columns(bases[0], MARGIN)
    strip_columns(own_at[1] + half_rows, MARGIN)
    strip_rows(-MARGIN, bases[0], MARGIN, 0, HALF)
    strip_rows(rows, own_at[1] + half_rows, MARGIN, MARGIN + half_rows, 0)
    for number in range(2):
        name = PACKED[number][0]
        lanes = lane_index(EXTRA)
        field[name][main, past] = jnp.where(
            lanes < OWN, field[name][0, past], rolled(field[name][main - 1, past], AT_HALO - LANES))
        field[name][main, past] = strip_value(number, rows + MARGIN, past.start, EXTRA, 0, 0)
        for t in range(tiles):
            field[name][t, other_past] = field[name][t, bases[1] + 2 * MARGIN : bases[1] + 2 * MARGIN + EXTRA]
    for name in ("plus", "minus", "twice"):
        for t in range(tiles):
            for base in bases:
                field[name][t, base - PAD : base] = jnp.zeros((PAD, LANES), jnp.float32)

    u, v, plus, minus, twice = (field[name] for name in ("u", "v", "plus", "minus", "twice"))
    u_next, v_next = field["u_next"], field["v_next"]
    def ahead(values):
        turned = [rolled(value, -1) for value in values]
        at_end = lane_index(values[0].shape[0]) == LANES - 1
        return [jnp.where(at_end, turned[(t + 1) % main], turned[t]) for t in range(main)] + turned[main:]

    def behind(values):
        turned = [rolled(value, 1) for value in values]
        at_start = lane_index(values[0].shape[0]) == 0
        return [jnp.where(at_start, turned[t - 1 if t else main - 1], turned[t]) for t in range(main)] + turned[main:]

    def gradients(start, count):
        add, sub, add_s, sub_s = [], [], [], []
        at, after = pl.ds(start, count), pl.ds(start + 1, count)
        for t in range(tiles):
            u0, u1, v0, v1 = u[t, at], u[t, after], v[t, at], v[t, after]
            a, b, c, d = u0 + u1, u1 - u0, v0 + v1, v1 - v0
            add.append(a + d)
            sub.append(a - d)
            add_s.append(b + c)
            sub_s.append(b - c)
        return add, sub, add_s, sub_s

    def stress_sums(start):
        at, before = pl.ds(start, STEP), pl.ds(start - 1, STEP)
        e_near, e_far, n_near, n_far = [], [], [], []
        for t in range(tiles):
            p1, p0 = plus[t, at], plus[t, before]
            m1, m0 = minus[t, at], minus[t, before]
            s1, s0 = twice[t, at], twice[t, before]
            a, d, b, e = p0 + p1, s1 - s0, s0 + s1, m1 - m0
            e_near.append(a + d)
            e_far.append(a - d)
            n_near.append(b + e)
            n_far.append(b - e)
        return e_near, e_far, n_near, n_far

    def stress_rows(start, growth):
        at, after = pl.ds(start, STEP), pl.ds(start + 1, STEP)
        for t in range(tiles):
            u0, u1, v0, v1 = u[t, at], u[t, after], v[t, at], v[t, after]
            u2, u3, v2, v3 = u_next[t, at], u_next[t, after], v_next[t, at], v_next[t, after]
            along, across_y = (u2 + u3) - (u0 + u1), (v1 - v0) + (v3 - v2)
            div, tension = along + across_y, along - across_y
            shear = ((u1 - u0) + (u3 - u2)) + ((v2 + v3) - (v0 + v1))
            square = div * div + (1.0 / ECCENTRICITY_SQUARED) * (tension * tension + shear * shear)
            inverse = lax.rsqrt(jnp.maximum(square, TINY))
            weight = (field["pressure"][t, at] * growth) * jnp.minimum(inverse, 1.0)
            quarter = weight * (1.0 / ECCENTRICITY_SQUARED)
            change = weight * (div - square * inverse)
            other = quarter * tension
            plus[t, at] = plus[t, at] + (change + other)
            minus[t, at] = minus[t, at] + (change - other)
            twice[t, at] = twice[t, at] + quarter * shear

    def velocity_rows(start, scale):
        at = pl.ds(start, STEP)
        for t in range(tiles):
            ce, cn = field["ce"][t, at], field["cn"][t, at]
            de, dn = u[t, at] - ce, v[t, at] - cn
            square = de * de + dn * dn
            drag = square * lax.rsqrt(jnp.maximum(square, TINY))
            heavy, turn = field["inertia"][t, at], field["turning"][t, at]
            diag = heavy + drag
            force_e = (field["e_near"][t, at] - field["e_back"][t, at]) * scale
            force_n = (field["n_near"][t, at] - field["n_back"][t, at]) * scale
            push_e = heavy * de + (force_e + field["ge"][t, at])
            push_n = heavy * dn + (force_n + field["gn"][t, at])
            inverse = lax.rsqrt(diag * diag + field["bound"][t, at])
            inverse = inverse * inverse
            u[t, at] = (diag * push_e + turn * push_n) * inverse + ce
            v[t, at] = (diag * push_n - turn * push_e) * inverse + cn

    def run(count, base, carried):
        last = base + reach - STEP

        def step(_, carried):
            at_g, at_h, at_s, at_f, at_v, growth, growth_h, growth_s, scale, scale_h, scale_s, scale_f, scale_v = carried
            at_g, at_h, at_s, at_f, at_v = (pl.multiple_of(each, 8) for each in (at_g, at_h, at_s, at_f, at_v))

            def keep(names, values, start):
                for name, each in zip(names, values):
                    for t in range(tiles):
                        field[name][t, pl.ds(start, STEP)] = each[t]

            moved = [ahead([ref[t, pl.ds(at_g, STEP)] for t in range(tiles)]) for ref in (u, v)]
            e_near, e_far, n_near, n_far = stress_sums(at_f)
            e_back, n_back = behind(e_far), behind(n_far)
            stress_rows(at_s, growth_s)
            velocity_rows(at_v, scale_v)
            keep(("u_next", "v_next"), moved, at_g)
            keep(("e_near", "n_near", "e_back", "n_back"), (e_near, n_near, e_back, n_back), at_f)
            wrap = at_g == last
            return (
                jnp.where(wrap, base, jnp.where(at_g == spare, spare, at_g + STEP)), at_g, at_h, at_s, at_f,
                jnp.where(wrap, growth * GAIN, growth), growth, growth_h,
                jnp.where(wrap, scale * (1.0 / GAIN), scale), scale, scale_h, scale_s, scale_f,
            )

        return lax.fori_loop(0, count, step, carried)

    def begin(at, carried):
        growth, scale = jnp.float32(GAIN), jnp.float32(0.25 / GAIN)
        return (jnp.int32(at),) + carried[1:5] + (growth,) + carried[6:8] + (scale,) + carried[9:]

    shrink = 0.5 * GAIN**-SUBCYCLES

    def merged(values):
        lanes = lane_index(values[0].shape[0])
        on_left, on_right = lanes < MARGIN, lanes >= LANES - MARGIN - 2
        values = list(values)
        values[0] = jnp.where(on_left, values[main], values[0])
        values[main - 1] = jnp.where(on_right, rolled(values[main], LANES - AT_HALO), values[main - 1])
        return values[:main]

    def finish_conc(start, row, count):
        add, sub, _, _ = gradients(start, count)
        add_next = ahead(add)
        div = merged([add_next[t] - sub[t] for t in range(tiles)])
        for t in range(main):
            c = slice(t * LANES, (t + 1) * LANES)
            value = sconc[pl.ds(MARGIN + row, count), c]
            conc_out[pl.ds(row, count), c] = jnp.clip(value - value * (0.5 * div[t]), 0.0, 1.0)

    def finish(start, row, count):
        here, at = pl.ds(start, count), pl.ds(row, count)
        east, north, one, two, three = (
            merged([ref[t, here] for t in range(tiles)]) for ref in (u, v, plus, minus, twice)
        )
        for t in range(main):
            c = slice(t * LANES, (t + 1) * LANES)
            vel_out[0, at, c] = east[t]
            vel_out[1, at, c] = north[t]
            stress_out[0, at, c] = (one[t] + two[t]) * shrink
            stress_out[1, at, c] = (one[t] - two[t]) * shrink
            stress_out[2, at, c] = three[t] * shrink
        finish_conc(start, row, count)

    def finish_half(half):
        def body(block, _):
            start = block * CHUNK
            finish(
                pl.multiple_of(jnp.where(half == 0, own_at[0], own_at[1]) + start, 8),
                pl.multiple_of(half * half_rows + start, 8), CHUNK,
            )
            return 0

        lax.fori_loop(0, half_rows // CHUNK, body, 0)

    early = (1 - me) if ens_count == 2 else jnp.int32(0)
    late = 1 - early
    share = rows // ens_count
    swaps = []
    for step, peer in enumerate(peers):
        part_of = pl.ds(pl.multiple_of(peer * share, 8), share)
        swaps.append(remote(
            vel_out.at[:, part_of], landing.at[step, 1:3], send_e, recv_e, 2 * step, {"ens": peer}))
        swaps.append(remote(
            conc_out.at[part_of], landing.at[step, 0], send_e, recv_e, 2 * step + 1, {"ens": peer}))

    for beyond_domain in (past, other_past):
        for ref, target in ((u, u_next), (v, v_next)):
            for t, each in enumerate(ahead([ref[t, beyond_domain] for t in range(tiles)])):
                target[t, beyond_domain] = each
    steps, lag = SUBCYCLES * (reach // STEP), 4
    one, empty = jnp.float32(1.0), jnp.int32(spare)
    first = jnp.where(early == 0, bases[0], bases[1])
    second = jnp.where(late == 0, bases[0], bases[1])
    carried = begin(first, (empty,) * 5 + (one,) * 8)
    carried = run(steps, first, carried)
    carried = run(lag, second, begin(second, carried))
    finish_half(early)
    if ens_count == 2:
        for each in swaps:
            each.start()
    carried = run(steps - lag, second, carried)
    run(lag, spare, begin(spare, carried))
    finish_half(late)
    if ens_count != 2:
        for each in swaps:
            each.start()
    for each in across:
        each.wait_send()

    @pl.when(has_lo)
    def _():
        for each in down + corner_lo:
            each.wait_send()

    @pl.when(has_hi)
    def _():
        for each in up + corner_hi:
            each.wait_send()

    for each in swaps:
        each.wait_recv()
    for each in swaps:
        each.wait_send()


def write_kernel(count, vel, stress, conc, landing, vel_out, stress_out, mean_out, spread_out, mean, spread, sems):
    copies = [
        pltpu.make_async_copy(vel, vel_out, sems.at[0]),
        pltpu.make_async_copy(stress, stress_out, sems.at[1]),
    ]
    for each in copies:
        each.start()
    share = mean.shape[1]
    own = pl.ds(pl.multiple_of(lax.axis_index("ens") * share, 8), share)
    for f in range(3):
        values = [conc[own] if f == 0 else vel[f - 1, own]]
        values += [landing[step, f] for step in range(count - 1)]
        average = functools.reduce(jnp.add, values) / count
        mean[f] = average
        spread[f] = functools.reduce(jnp.add, [(v - average) * (v - average) for v in values]) / count
    more = [
        pltpu.make_async_copy(mean, mean_out, sems.at[2]),
        pltpu.make_async_copy(spread, spread_out, sems.at[3]),
    ]
    for each in more:
        each.start()
    for each in copies + more:
        each.wait()


def solution(mesh):
    gx_count, gy_count, ens_count = mesh.shape["gx"], mesh.shape["gy"], mesh.shape["ens"]
    f32 = jnp.float32

    def vmem(*shape, dtype=f32):
        return pltpu.VMEM(shape, dtype)

    def specs(count, space):
        return [pl.BlockSpec(memory_space=space)] * count

    def body(velocity, stress, thickness, concentration, node_mass, wind, current, mask, ice):
        rows, cols = mask.shape
        share = rows // ens_count
        tiles = cols // LANES + 1
        block_rows, block_cols = ice.shape[1:]
        tall = rows + 2 * MARGIN
        total = -(-(5 * PAD + 2 * (rows // 2 + 2 * MARGIN) + STEP + PAD) // 32) * 32
        shape = lambda *dims: jax.ShapeDtypeStruct(dims, f32)
        dma = lambda count: pltpu.SemaphoreType.DMA((count,))
        state = pl.pallas_call(
            functools.partial(step_kernel, (gx_count, gy_count, ens_count)),
            name="subcycles",
            out_shape=(
                shape(2, rows, cols),
                shape(3, rows, cols),
                shape(rows, cols),
                shape(ens_count - 1, 3, share, cols),
            ),
            in_specs=specs(9, pltpu.HBM),
            out_specs=tuple(specs(4, pltpu.VMEM)),
            scratch_shapes=[vmem(tiles, total, LANES)] * len(MAIN_FIELDS)
            + [
                vmem(2, tall + EXTRA, cols),
                vmem(3, tall, cols),
                vmem(tall, cols),
                vmem(tall, cols),
                vmem(tall, cols),
                vmem(2, tall, cols),
                vmem(2, tall, cols),
                vmem(tall + EXTRA, cols, dtype=jnp.int32),
                vmem(3 * block_rows, block_cols, dtype=jnp.int32),
                vmem(24 * block_rows, cols),
                vmem(2, rows, LANES),
                vmem(2, rows // 2, LANES),
                vmem(2, tall + EXTRA, LANES),
                vmem(2, rows // 2 + 2 * MARGIN, LANES),
                dma(17), dma(18), dma(18), dma(4), dma(4), dma(8), dma(8),
                dma(2 * (ens_count - 1)), dma(2 * (ens_count - 1)),
            ],
            compiler_params=pltpu.CompilerParams(
                collective_id=0, has_side_effects=True, vmem_limit_bytes=28 << 20),
        )(*(pltpu.with_memory_space_constraint(each, pltpu.HBM) for each in (
            velocity[0], stress[0], thickness[0], concentration[0], node_mass[0], wind[0], current[0], mask, ice[0])))
        vel_out, stress_out, mean, spread = pl.pallas_call(
            functools.partial(write_kernel, ens_count),
            name="write",
            out_shape=(shape(2, rows, cols), shape(3, rows, cols), shape(3, share, cols), shape(3, share, cols)),
            in_specs=specs(4, pltpu.VMEM),
            out_specs=tuple(specs(4, pltpu.HBM)),
            scratch_shapes=[vmem(3, share, cols), vmem(3, share, cols), dma(4)],
            compiler_params=pltpu.CompilerParams(vmem_limit_bytes=4 << 20),
        )(*state)
        return vel_out[None], stress_out[None], mean, spread

    grid = P("ens", "gy", "gx")
    pair = P("ens", None, "gy", "gx")
    split = P(None, ("gy", "ens"), "gx")
    return jax.shard_map(
        body,
        mesh=mesh,
        in_specs=(pair, pair, grid, grid, grid, pair, pair, P("gy", "gx"), grid),
        out_specs=(pair, pair, split, split),
        check_vma=False,
    )
```

```python
import functools

import jax
import jax.numpy as jnp
from jax import lax
from jax.experimental import pallas as pl
from jax.experimental.pallas import tpu as pltpu
from jax.sharding import PartitionSpec as P

SUBCYCLES = 16
BLOCK = 32

TIME_STEP = 0.5
RELAX_RATE = 0.25
ECCENTRICITY_SQUARED = 4.0
CORIOLIS_TOP = 1.0
STRENGTH_DECAY = 20.0

MESH = pl.DeviceIdType.MESH
LANES = 128
TINY = 1.1754944e-38
GAIN = 1.0 + RELAX_RATE

MARGIN = SUBCYCLES
EXTRA = 8
PAD = 8
CHUNK = 64
STEP = 32

PACKED = (
    ("u", MARGIN + 1), ("v", MARGIN + 1), ("plus", MARGIN), ("minus", MARGIN), ("twice", MARGIN),
    ("pressure", MARGIN), ("inertia", MARGIN),
    ("ge", MARGIN), ("gn", MARGIN), ("ce", MARGIN), ("cn", MARGIN),
)
WHOLE = 7
OFFSETS = []
for _i, (_, _w) in enumerate(PACKED):
    if _i == 0 or _i == WHOLE:
        OFFSETS.append(0)
    else:
        OFFSETS.append(OFFSETS[-1] + PACKED[_i - 1][1])
HALF = LANES // 2

OWN = 36
AT_RIGHT = 48
AT_HALO = AT_RIGHT + OWN
AT_LEFT = LANES - MARGIN

MAIN_FIELDS = (
    "u", "v", "plus", "minus", "twice", "pressure", "inertia", "turning",
    "ge", "gn", "ce", "cn", "bound", "re", "rn",
    "u_next", "v_next", "e_near", "n_near", "e_back", "n_back",
)


def lane_index(rows):
    return lax.broadcasted_iota(jnp.int32, (rows, LANES), 1)


def rolled(value, shift):
    shift = shift % LANES
    return value if shift == 0 else pltpu.roll(value, shift, 1)


def step_kernel(sizes, *refs):
    gx_count, gy_count, ens_count = sizes
    inputs, refs = refs[:9], refs[9:]
    (vel_out, stress_out, conc_out, landing), refs = refs[:4], refs[4:]
    arrays, refs = refs[: len(MAIN_FIELDS)], refs[len(MAIN_FIELDS) :]
    (svel, sstress, sthick, sconc, smass, swind, scur, smask, sice, expand), refs = refs[:10], refs[10:]
    (out_a, out_b, in_a, in_b, load_sem, send_y, recv_y, send_x, recv_x, send_d, recv_d, send_e, recv_e) = refs
    field = dict(zip(MAIN_FIELDS, arrays))
    stages = (svel, sstress, sthick, sconc, smass, swind, scur, smask)
    rows, cols = conc_out.shape
    main = cols // LANES
    tiles = main + 1
    blocks = rows // BLOCK
    half_rows = rows // 2
    reach = half_rows + 2 * MARGIN
    bases = (PAD, 3 * PAD + reach)
    first_rows = (-MARGIN, half_rows - MARGIN)
    spare = 5 * PAD + 2 * reach
    gx, gy, me = lax.axis_index("gx"), lax.axis_index("gy"), lax.axis_index("ens")
    right, left = lax.rem(gx + 1, gx_count), lax.rem(gx + gx_count - 1, gx_count)
    has_lo, has_hi = gy > 0, gy < gy_count - 1
    lower, upper = jnp.maximum(gy - 1, 0), jnp.minimum(gy + 1, gy_count - 1)
    peers = [lax.rem(me + step, ens_count) for step in range(1, ens_count)]

    barrier = pltpu.get_barrier_semaphore()

    def greet(**where):
        pl.semaphore_signal(barrier, inc=1, device_id=where, device_id_type=MESH)

    greet(gx=left)
    greet(gx=right)
    for peer in peers:
        greet(ens=peer)
    for there, row in ((has_lo, lower), (has_hi, upper)):
        @pl.when(there)
        def _(row=row):
            greet(gy=row)
            greet(gy=row, gx=left)
            greet(gy=row, gx=right)

    def at_rows(ref, where):
        return ref.at[:, where] if len(ref.shape) == 3 else ref.at[where]

    loads = [[
        pltpu.make_async_copy(
            at_rows(source, slice(half * half_rows, (half + 1) * half_rows)),
            at_rows(stage, slice(MARGIN + half * half_rows, MARGIN + (half + 1) * half_rows)),
            load_sem.at[8 * half + number],
        )
        for number, (source, stage) in enumerate(zip(inputs, stages))
    ] for half in range(2)]
    loads[0].append(pltpu.make_async_copy(inputs[8], sice.at[blocks : 2 * blocks], load_sem.at[16]))
    for each in loads[0] + loads[1]:
        each.start()

    def remote(source, target, sends, receives, number, where):
        return pltpu.make_async_remote_copy(
            src_ref=source, dst_ref=target, send_sem=sends.at[number], recv_sem=receives.at[number],
            device_id=where, device_id_type=MESH,
        )

    down, up = [], []
    for number, (source, stage) in enumerate(zip(inputs, stages)):
        extra = EXTRA if number in (0, 7) else 0
        down.append(remote(
            at_rows(source, slice(0, MARGIN + extra)),
            at_rows(stage, slice(MARGIN + rows, 2 * MARGIN + rows + extra)),
            send_y, recv_y, number, {"gy": lower},
        ))
        up.append(remote(
            at_rows(source, slice(rows - MARGIN, rows)),
            at_rows(stage, slice(0, MARGIN)),
            send_y, recv_y, 9 + number, {"gy": upper},
        ))
    down.append(remote(inputs[8], sice.at[2 * blocks : 3 * blocks], send_y, recv_y, 8, {"gy": lower}))
    up.append(remote(inputs[8], sice.at[0:blocks], send_y, recv_y, 17, {"gy": upper}))

    others = has_lo.astype(jnp.int32) + has_hi.astype(jnp.int32)
    pl.semaphore_wait(barrier, 2 + (ens_count - 1) + 3 * others)

    @pl.when(has_lo)
    def _():
        for each in down:
            each.start()

    @pl.when(has_hi)
    def _():
        for each in up:
            each.start()

    block_cols = sice.shape[1]
    spread = (
        lax.broadcasted_iota(jnp.int32, (block_cols, cols), 1) // BLOCK
        == lax.broadcasted_iota(jnp.int32, (block_cols, cols), 0)
    ).astype(jnp.float32)

    repeat = (
        lax.broadcasted_iota(jnp.int32, (8 * blocks, blocks), 0) // 8
        == lax.broadcasted_iota(jnp.int32, (8 * blocks, blocks), 1)
    ).astype(jnp.float32)

    def expand_ice(part):
        flags = sice[part * blocks : (part + 1) * blocks].astype(jnp.float32)
        flags = jnp.dot(repeat, flags, preferred_element_type=jnp.float32)
        expand[8 * part * blocks : 8 * (part + 1) * blocks] = jnp.dot(
            flags, spread, preferred_element_type=jnp.float32)

    def convert(start, count, ice_row, target):
        at = pl.ds(start, count)
        to = pl.ds(target, count)
        row = lax.broadcasted_iota(jnp.int32, (count, LANES), 0) + (gy * rows + (start - MARGIN))
        coriolis = CORIOLIS_TOP * (row.astype(jnp.float32) + 0.5) / (rows * gy_count)
        sent = []
        for t in range(main):
            c = slice(t * LANES, (t + 1) * LANES)
            present = jnp.concatenate([expand[pl.ds(ice_row, 8), c]] * (count // 8))
            alive = smask[at, c].astype(jnp.float32) * present
            one, two = sstress[0, at, c], sstress[1, at, c]
            factor = RELAX_RATE * 0.5 / GAIN
            heavy = smass[at, c]
            heavy = jnp.where(heavy == 0.0, 1.0, heavy)
            turn = coriolis * heavy
            ce, cn = scur[0, at, c], scur[1, at, c]
            value = {
                "u": svel[0, at, c] * alive,
                "v": svel[1, at, c] * alive,
                "plus": one + two,
                "minus": one - two,
                "twice": 2.0 * sstress[2, at, c],
                "pressure": factor * sthick[at, c] * jnp.exp(-STRENGTH_DECAY * (1.0 - sconc[at, c])),
                "inertia": heavy / TIME_STEP,
                "turning": turn,
                "bound": jnp.where(alive == 0.0, jnp.inf, turn * turn),
                "ge": swind[0, at, c] + turn * cn,
                "gn": swind[1, at, c] - turn * ce,
                "ce": alive * ce,
                "cn": alive * cn,
            }
            value["re"], value["rn"] = value["u"] - value["ce"], value["v"] - value["cn"]
            for name, each in value.items():
                field[name][t, to] = each
            value["inertia"] = value["inertia"] * alive
            sent.append(value)
        return sent

    whole, part = range(WHOLE), range(WHOLE, len(PACKED))

    def packed(sent, fields, shift, east, west):
        lanes = lane_index(east.shape[0])
        for number in fields:
            name, width = PACKED[number]
            start = OFFSETS[number] + shift
            here = jnp.logical_and(lanes >= start, lanes < start + width)
            east = jnp.where(here, rolled(sent[main - 1][name], start - (LANES - MARGIN)), east)
            west = jnp.where(here, rolled(sent[0][name], start), west)
        return east, west

    own_at = (PAD + MARGIN, bases[1] + MARGIN)
    for half in range(2):
        for each in loads[half]:
            each.wait()
        if half == 0:
            expand_ice(1)

        def convert_own(block, _, half=half):
            start = pl.multiple_of(half * half_rows + block * BLOCK, 8)
            sent = convert(
                MARGIN + start, BLOCK, pl.multiple_of(8 * (blocks + half * blocks // 2 + block), 8),
                pl.multiple_of(own_at[half] + block * BLOCK, 8),
            )
            zero = jnp.zeros((BLOCK, LANES), jnp.float32)
            to, to_half = pl.ds(start, BLOCK), pl.ds(pl.multiple_of(block * BLOCK, 8), BLOCK)
            out_a[0, to], out_a[1, to] = packed(sent, whole, 0, zero, zero)
            before = (out_b[0, to_half], out_b[1, to_half]) if half else (zero, zero)
            out_b[0, to_half], out_b[1, to_half] = packed(sent, part, half * HALF, *before)
            return 0

        lax.fori_loop(0, blocks // 2, convert_own, 0)

    def message(name, tile, at):
        value = field[name][tile, at]
        return jnp.where(field["bound"][tile, at] == jnp.inf, 0.0, value) if name == "inertia" else value

    sides = (right, left)
    across, corner_lo, corner_hi = [], [], []
    for side, to in enumerate(sides):
        across.append(remote(
            out_a.at[side], in_a.at[side, MARGIN : MARGIN + rows], send_x, recv_x, 2 * side, {"gx": to}))
        across.append(remote(
            out_b.at[side], in_b.at[side, MARGIN : MARGIN + half_rows], send_x, recv_x, 2 * side + 1, {"gx": to}))
        lo, hi = {"gx": to, "gy": lower}, {"gx": to, "gy": upper}
        corner_lo.append(remote(
            out_a.at[side, 0 : MARGIN + EXTRA],
            in_a.at[side, MARGIN + rows : 2 * MARGIN + rows + EXTRA],
            send_d, recv_d, 4 * side, lo))
        corner_lo.append(remote(
            out_b.at[side, 0:MARGIN],
            in_b.at[side, MARGIN + half_rows : 2 * MARGIN + half_rows],
            send_d, recv_d, 4 * side + 1, lo))
        corner_hi.append(remote(
            out_a.at[side, rows - MARGIN : rows], in_a.at[side, 0:MARGIN],
            send_d, recv_d, 4 * side + 2, hi))
        corner_hi.append(remote(
            out_b.at[side, half_rows - MARGIN : half_rows], in_b.at[side, 0:MARGIN],
            send_d, recv_d, 4 * side + 3, hi))
    for each in across:
        each.start()

    @pl.when(has_lo)
    def _():
        for each in corner_lo:
            each.start()

    @pl.when(has_hi)
    def _():
        for each in corner_hi:
            each.start()

    convert(MARGIN + half_rows, MARGIN, 8 * (blocks + blocks // 2), own_at[0] + half_rows)
    convert(half_rows, MARGIN, 8 * (blocks + blocks // 2 - 1), bases[1])

    def strip_columns(target, count):
        at = pl.ds(target, count)
        lanes = lane_index(count)
        for name, _ in PACKED:
            field[name][main, at] = jnp.where(
                lanes < OWN, message(name, 0, at), rolled(message(name, main - 1, at), AT_HALO - LANES))

    for half in range(2):
        def own_columns(block, _, half=half):
            strip_columns(pl.multiple_of(own_at[half] + block * CHUNK, 8), CHUNK)
            return 0

        lax.fori_loop(0, half_rows // CHUNK, own_columns, 0)
    strip_columns(own_at[0] + half_rows, MARGIN)
    strip_columns(bases[1], MARGIN)

    @pl.when(has_lo)
    def _():
        for each in up:
            each.wait_recv()

    @pl.when(jnp.logical_not(has_lo))
    def _():
        for stage in stages:
            for index in range(stage.shape[0]) if len(stage.shape) == 3 else (None,):
                view = stage if index is None else stage.at[index]
                view[0:MARGIN] = jnp.zeros((MARGIN, cols), stage.dtype)
        sice[0:blocks] = jnp.zeros((blocks, block_cols), jnp.int32)

    @pl.when(has_hi)
    def _():
        for each in down:
            each.wait_recv()

    @pl.when(jnp.logical_not(has_hi))
    def _():
        for stage in stages:
            count = stage.shape[-2] - MARGIN - rows
            for index in range(stage.shape[0]) if len(stage.shape) == 3 else (None,):
                view = stage if index is None else stage.at[index]
                view[MARGIN + rows : MARGIN + rows + count] = jnp.zeros((count, cols), stage.dtype)
        sice[2 * blocks : 3 * blocks] = jnp.zeros((blocks, block_cols), jnp.int32)

    expand_ice(0)
    expand_ice(2)
    convert(0, MARGIN, 8 * (blocks - 1), bases[0])
    convert(MARGIN + rows, MARGIN, 16 * blocks, own_at[1] + half_rows)
    beyond = slice(2 * MARGIN + rows, 2 * MARGIN + rows + EXTRA)
    past = slice(bases[1] + reach, bases[1] + reach + EXTRA)
    other_past = slice(bases[0] + reach, bases[0] + reach + EXTRA)
    for t in range(main):
        c = slice(t * LANES, (t + 1) * LANES)
        alive = smask[beyond, c].astype(jnp.float32) * expand[16 * blocks : 16 * blocks + 8, c]
        field["u"][t, past] = svel[0, beyond, c] * alive
        field["v"][t, past] = svel[1, beyond, c] * alive

    for each in across:
        each.wait_recv()

    @pl.when(has_lo)
    def _():
        for each in corner_hi:
            each.wait_recv()

    @pl.when(jnp.logical_not(has_lo))
    def _():
        for side in range(2):
            in_a[side, 0:MARGIN] = jnp.zeros((MARGIN, LANES), jnp.float32)
            in_b[side, 0:MARGIN] = jnp.zeros((MARGIN, LANES), jnp.float32)

    @pl.when(has_hi)
    def _():
        for each in corner_lo:
            each.wait_recv()

    @pl.when(jnp.logical_not(has_hi))
    def _():
        for side in range(2):
            in_a[side, MARGIN + rows :] = jnp.zeros((MARGIN + EXTRA, LANES), jnp.float32)
            in_b[side, MARGIN + half_rows :] = jnp.zeros((MARGIN, LANES), jnp.float32)

    def strip_value(number, row, target, count, half_start, half_lane):
        name, width = PACKED[number]
        lanes = lane_index(count)
        if number < WHOLE:
            arrived, there, lane = in_a, pl.ds(row + MARGIN, count), OFFSETS[number]
        else:
            arrived, there, lane = in_b, pl.ds(half_start, count), OFFSETS[number] + half_lane
        value = jnp.where(lanes < AT_HALO + width, rolled(arrived[1, there], AT_HALO - lane), 0.0)
        value = jnp.where(lanes < AT_HALO, field[name][main, pl.ds(target, count)], value)
        return jnp.where(lanes >= AT_LEFT, rolled(arrived[0, there], AT_LEFT - lane), value)

    def strip_rows(first, target, count, half_start, half_lane):
        at = pl.ds(target, count)
        value = {
            name: strip_value(number, first, target, count, half_start, half_lane)
            for number, (name, _) in enumerate(PACKED)
        }
        row = lax.broadcasted_iota(jnp.int32, (count, LANES), 0) + (gy * rows + first)
        coriolis = CORIOLIS_TOP * (row.astype(jnp.float32) + 0.5) / (rows * gy_count)
        empty = value["inertia"] == 0.0
        heavy = jnp.where(empty, 1.0 / TIME_STEP, value["inertia"])
        value["inertia"] = heavy
        value["turning"] = coriolis * (heavy * TIME_STEP)
        value["bound"] = jnp.where(empty, jnp.inf, value["turning"] * value["turning"])
        value["re"], value["rn"] = value["u"] - value["ce"], value["v"] - value["cn"]
        for name, each in value.items():
            field[name][main, at] = each

    for half in range(2):
        def strip_own(block, _, half=half):
            start = pl.multiple_of(block * CHUNK, 8)
            strip_rows(half * half_rows + start, pl.multiple_of(own_at[half] + start, 8), CHUNK,
                       MARGIN + start, half * HALF)
            return 0

        lax.fori_loop(0, half_rows // CHUNK, strip_own, 0)
    strip_rows(half_rows, own_at[0] + half_rows, MARGIN, MARGIN, HALF)
    strip_rows(half_rows - MARGIN, bases[1], MARGIN, half_rows, 0)
    strip_columns(bases[0], MARGIN)
    strip_columns(own_at[1] + half_rows, MARGIN)
    strip_rows(-MARGIN, bases[0], MARGIN, 0, HALF)
    strip_rows(rows, own_at[1] + half_rows, MARGIN, MARGIN + half_rows, 0)
    for number in range(2):
        name = PACKED[number][0]
        lanes = lane_index(EXTRA)
        field[name][main, past] = jnp.where(
            lanes < OWN, field[name][0, past], rolled(field[name][main - 1, past], AT_HALO - LANES))
        field[name][main, past] = strip_value(number, rows + MARGIN, past.start, EXTRA, 0, 0)
        for t in range(tiles):
            field[name][t, other_past] = field[name][t, bases[1] + 2 * MARGIN : bases[1] + 2 * MARGIN + EXTRA]
    for name in ("plus", "minus", "twice"):
        for t in range(tiles):
            for base in bases:
                field[name][t, base - PAD : base] = jnp.zeros((PAD, LANES), jnp.float32)

    u, v, plus, minus, twice = (field[name] for name in ("u", "v", "plus", "minus", "twice"))
    u_next, v_next = field["u_next"], field["v_next"]
    def ahead(values):
        turned = [rolled(value, -1) for value in values]
        at_end = lane_index(values[0].shape[0]) == LANES - 1
        return [jnp.where(at_end, turned[(t + 1) % main], turned[t]) for t in range(main)] + turned[main:]

    def behind(values):
        turned = [rolled(value, 1) for value in values]
        at_start = lane_index(values[0].shape[0]) == 0
        return [jnp.where(at_start, turned[t - 1 if t else main - 1], turned[t]) for t in range(main)] + turned[main:]

    def gradients(start, count):
        add, sub, add_s, sub_s = [], [], [], []
        at, after = pl.ds(start, count), pl.ds(start + 1, count)
        for t in range(tiles):
            u0, u1, v0, v1 = u[t, at], u[t, after], v[t, at], v[t, after]
            a, b, c, d = u0 + u1, u1 - u0, v0 + v1, v1 - v0
            add.append(a + d)
            sub.append(a - d)
            add_s.append(b + c)
            sub_s.append(b - c)
        return add, sub, add_s, sub_s

    def stress_sums(start):
        at, before = pl.ds(start, STEP), pl.ds(start - 1, STEP)
        e_near, e_far, n_near, n_far = [], [], [], []
        for t in range(tiles):
            p1, p0 = plus[t, at], plus[t, before]
            m1, m0 = minus[t, at], minus[t, before]
            s1, s0 = twice[t, at], twice[t, before]
            a, d, b, e = p0 + p1, s1 - s0, s0 + s1, m1 - m0
            e_near.append(a + d)
            e_far.append(a - d)
            n_near.append(b + e)
            n_far.append(b - e)
        return e_near, e_far, n_near, n_far

    def stress_rows(start, growth):
        for t, piece in [(t, piece) for t in range(tiles) for piece in range(0, STEP, 8)]:
            at, after = pl.ds(start + piece, 8), pl.ds(start + piece + 1, 8)
            u0, u1, v0, v1 = u[t, at], u[t, after], v[t, at], v[t, after]
            u2, u3, v2, v3 = u_next[t, at], u_next[t, after], v_next[t, at], v_next[t, after]
            along, across_y = (u2 + u3) - (u0 + u1), (v1 - v0) + (v3 - v2)
            div, tension = along + across_y, along - across_y
            shear = ((u1 - u0) + (u3 - u2)) + ((v2 + v3) - (v0 + v1))
            square = div * div + (1.0 / ECCENTRICITY_SQUARED) * (tension * tension + shear * shear)
            inverse = lax.rsqrt(jnp.maximum(square, TINY))
            weight = (field["pressure"][t, at] * growth) * jnp.minimum(inverse, 1.0)
            quarter = weight * (1.0 / ECCENTRICITY_SQUARED)
            change = weight * (div - square * inverse)
            other = quarter * tension
            plus[t, at] = plus[t, at] + (change + other)
            minus[t, at] = minus[t, at] + (change - other)
            twice[t, at] = twice[t, at] + quarter * shear

    def velocity_rows(start, scale):
        for t, piece in [(t, piece) for t in range(tiles) for piece in range(0, STEP, 8)]:
            at = pl.ds(start + piece, 8)
            de, dn = field["re"][t, at], field["rn"][t, at]
            square = de * de + dn * dn
            drag = square * lax.rsqrt(jnp.maximum(square, TINY))
            heavy, turn = field["inertia"][t, at], field["turning"][t, at]
            diag = heavy + drag
            force_e = (field["e_near"][t, at] - field["e_back"][t, at]) * scale
            force_n = (field["n_near"][t, at] - field["n_back"][t, at]) * scale
            push_e = heavy * de + (force_e + field["ge"][t, at])
            push_n = heavy * dn + (force_n + field["gn"][t, at])
            inverse = lax.rsqrt(diag * diag + field["bound"][t, at])
            inverse = inverse * inverse
            de = (diag * push_e + turn * push_n) * inverse
            dn = (diag * push_n - turn * push_e) * inverse
            field["re"][t, at], field["rn"][t, at] = de, dn
            u[t, at] = de + field["ce"][t, at]
            v[t, at] = dn + field["cn"][t, at]

    def run(count, base, carried):
        last = base + reach - STEP

        def step(_, carried):
            at_g, at_h, at_s, at_f, at_v, growth, growth_h, growth_s, scale, scale_h, scale_s, scale_f, scale_v = carried
            at_g, at_h, at_s, at_f, at_v = (pl.multiple_of(each, 8) for each in (at_g, at_h, at_s, at_f, at_v))

            def keep(names, values, start):
                for name, each in zip(names, values):
                    for t in range(tiles):
                        field[name][t, pl.ds(start, STEP)] = each[t]

            moved = [ahead([ref[t, pl.ds(at_g, STEP)] for t in range(tiles)]) for ref in (u, v)]
            e_near, e_far, n_near, n_far = stress_sums(at_f)
            e_back, n_back = behind(e_far), behind(n_far)
            stress_rows(at_s, growth_s)
            velocity_rows(at_v, scale_v)
            keep(("u_next", "v_next"), moved, at_g)
            keep(("e_near", "n_near", "e_back", "n_back"), (e_near, n_near, e_back, n_back), at_f)
            wrap = at_g == last
            return (
                jnp.where(wrap, base, jnp.where(at_g == spare, spare, at_g + STEP)), at_g, at_h, at_s, at_f,
                jnp.where(wrap, growth * GAIN, growth), growth, growth_h,
                jnp.where(wrap, scale * (1.0 / GAIN), scale), scale, scale_h, scale_s, scale_f,
            )

        return lax.fori_loop(0, count, step, carried)

    def begin(at, carried):
        growth, scale = jnp.float32(GAIN), jnp.float32(0.25 / GAIN)
        return (jnp.int32(at),) + carried[1:5] + (growth,) + carried[6:8] + (scale,) + carried[9:]

    shrink = 0.5 * GAIN**-SUBCYCLES

    def merged(values):
        lanes = lane_index(values[0].shape[0])
        on_left, on_right = lanes < MARGIN, lanes >= LANES - MARGIN - 2
        values = list(values)
        values[0] = jnp.where(on_left, values[main], values[0])
        values[main - 1] = jnp.where(on_right, rolled(values[main], LANES - AT_HALO), values[main - 1])
        return values[:main]

    def finish_conc(start, row, count):
        add, sub, _, _ = gradients(start, count)
        add_next = ahead(add)
        div = merged([add_next[t] - sub[t] for t in range(tiles)])
        for t in range(main):
            c = slice(t * LANES, (t + 1) * LANES)
            value = sconc[pl.ds(MARGIN + row, count), c]
            conc_out[pl.ds(row, count), c] = jnp.clip(value - value * (0.5 * div[t]), 0.0, 1.0)

    def finish(start, row, count):
        here, at = pl.ds(start, count), pl.ds(row, count)
        east, north, one, two, three = (
            merged([ref[t, here] for t in range(tiles)]) for ref in (u, v, plus, minus, twice)
        )
        for t in range(main):
            c = slice(t * LANES, (t + 1) * LANES)
            vel_out[0, at, c] = east[t]
            vel_out[1, at, c] = north[t]
            stress_out[0, at, c] = (one[t] + two[t]) * shrink
            stress_out[1, at, c] = (one[t] - two[t]) * shrink
            stress_out[2, at, c] = three[t] * shrink
        finish_conc(start, row, count)

    def finish_half(half):
        def body(block, _):
            start = block * CHUNK
            finish(
                pl.multiple_of(jnp.where(half == 0, own_at[0], own_at[1]) + start, 8),
                pl.multiple_of(half * half_rows + start, 8), CHUNK,
            )
            return 0

        lax.fori_loop(0, half_rows // CHUNK, body, 0)

    early = (1 - me) if ens_count == 2 else jnp.int32(0)
    late = 1 - early
    share = rows // ens_count
    swaps = []
    for step, peer in enumerate(peers):
        part_of = pl.ds(pl.multiple_of(peer * share, 8), share)
        swaps.append(remote(
            vel_out.at[:, part_of], landing.at[step, 1:3], send_e, recv_e, 2 * step, {"ens": peer}))
        swaps.append(remote(
            conc_out.at[part_of], landing.at[step, 0], send_e, recv_e, 2 * step + 1, {"ens": peer}))

    for beyond_domain in (past, other_past):
        for ref, target in ((u, u_next), (v, v_next)):
            for t, each in enumerate(ahead([ref[t, beyond_domain] for t in range(tiles)])):
                target[t, beyond_domain] = each
    steps, lag = SUBCYCLES * (reach // STEP), 4
    one, empty = jnp.float32(1.0), jnp.int32(spare)
    first = jnp.where(early == 0, bases[0], bases[1])
    second = jnp.where(late == 0, bases[0], bases[1])
    carried = begin(first, (empty,) * 5 + (one,) * 8)
    carried = run(steps, first, carried)
    carried = run(lag, second, begin(second, carried))
    finish_half(early)
    if ens_count == 2:
        for each in swaps:
            each.start()
    carried = run(steps - lag, second, carried)
    run(lag, spare, begin(spare, carried))
    finish_half(late)
    if ens_count != 2:
        for each in swaps:
            each.start()
    for each in across:
        each.wait_send()

    @pl.when(has_lo)
    def _():
        for each in down + corner_lo:
            each.wait_send()

    @pl.when(has_hi)
    def _():
        for each in up + corner_hi:
            each.wait_send()

    for each in swaps:
        each.wait_recv()
    for each in swaps:
        each.wait_send()


def write_kernel(count, vel, stress, conc, landing, vel_out, stress_out, mean_out, spread_out, mean, spread, sems):
    copies = [
        pltpu.make_async_copy(vel, vel_out, sems.at[0]),
        pltpu.make_async_copy(stress, stress_out, sems.at[1]),
    ]
    for each in copies:
        each.start()
    share = mean.shape[1]
    own = pl.ds(pl.multiple_of(lax.axis_index("ens") * share, 8), share)
    for f in range(3):
        values = [conc[own] if f == 0 else vel[f - 1, own]]
        values += [landing[step, f] for step in range(count - 1)]
        average = functools.reduce(jnp.add, values) / count
        mean[f] = average
        spread[f] = functools.reduce(jnp.add, [(v - average) * (v - average) for v in values]) / count
    more = [
        pltpu.make_async_copy(mean, mean_out, sems.at[2]),
        pltpu.make_async_copy(spread, spread_out, sems.at[3]),
    ]
    for each in more:
        each.start()
    for each in copies + more:
        each.wait()


def solution(mesh):
    gx_count, gy_count, ens_count = mesh.shape["gx"], mesh.shape["gy"], mesh.shape["ens"]
    f32 = jnp.float32

    def vmem(*shape, dtype=f32):
        return pltpu.VMEM(shape, dtype)

    def specs(count, space):
        return [pl.BlockSpec(memory_space=space)] * count

    def body(velocity, stress, thickness, concentration, node_mass, wind, current, mask, ice):
        rows, cols = mask.shape
        share = rows // ens_count
        tiles = cols // LANES + 1
        block_rows, block_cols = ice.shape[1:]
        tall = rows + 2 * MARGIN
        total = -(-(5 * PAD + 2 * (rows // 2 + 2 * MARGIN) + STEP + PAD) // 32) * 32
        shape = lambda *dims: jax.ShapeDtypeStruct(dims, f32)
        dma = lambda count: pltpu.SemaphoreType.DMA((count,))
        state = pl.pallas_call(
            functools.partial(step_kernel, (gx_count, gy_count, ens_count)),
            name="subcycles",
            out_shape=(
                shape(2, rows, cols),
                shape(3, rows, cols),
                shape(rows, cols),
                shape(ens_count - 1, 3, share, cols),
            ),
            in_specs=specs(9, pltpu.HBM),
            out_specs=tuple(specs(4, pltpu.VMEM)),
            scratch_shapes=[vmem(tiles, total, LANES)] * len(MAIN_FIELDS)
            + [
                vmem(2, tall + EXTRA, cols),
                vmem(3, tall, cols),
                vmem(tall, cols),
                vmem(tall, cols),
                vmem(tall, cols),
                vmem(2, tall, cols),
                vmem(2, tall, cols),
                vmem(tall + EXTRA, cols, dtype=jnp.int32),
                vmem(3 * block_rows, block_cols, dtype=jnp.int32),
                vmem(24 * block_rows, cols),
                vmem(2, rows, LANES),
                vmem(2, rows // 2, LANES),
                vmem(2, tall + EXTRA, LANES),
                vmem(2, rows // 2 + 2 * MARGIN, LANES),
                dma(17), dma(18), dma(18), dma(4), dma(4), dma(8), dma(8),
                dma(2 * (ens_count - 1)), dma(2 * (ens_count - 1)),
            ],
            compiler_params=pltpu.CompilerParams(
                collective_id=0, has_side_effects=True, vmem_limit_bytes=32 << 20),
        )(*(pltpu.with_memory_space_constraint(each, pltpu.HBM) for each in (
            velocity[0], stress[0], thickness[0], concentration[0], node_mass[0], wind[0], current[0], mask, ice[0])))
        vel_out, stress_out, mean, spread = pl.pallas_call(
            functools.partial(write_kernel, ens_count),
            name="write",
            out_shape=(shape(2, rows, cols), shape(3, rows, cols), shape(3, share, cols), shape(3, share, cols)),
            in_specs=specs(4, pltpu.VMEM),
            out_specs=tuple(specs(4, pltpu.HBM)),
            scratch_shapes=[vmem(3, share, cols), vmem(3, share, cols), dma(4)],
            compiler_params=pltpu.CompilerParams(vmem_limit_bytes=4 << 20),
        )(*state)
        return vel_out[None], stress_out[None], mean, spread

    grid = P("ens", "gy", "gx")
    pair = P("ens", None, "gy", "gx")
    split = P(None, ("gy", "ens"), "gx")
    return jax.shard_map(
        body,
        mesh=mesh,
        in_specs=(pair, pair, grid, grid, grid, pair, pair, P("gy", "gx"), grid),
        out_specs=(pair, pair, split, split),
        check_vma=False,
    )
```

```python
import functools

import jax
import jax.numpy as jnp
from jax import lax
from jax.experimental import pallas as pl
from jax.experimental.pallas import tpu as pltpu
from jax.sharding import PartitionSpec as P

SUBCYCLES = 16
BLOCK = 32

TIME_STEP = 0.5
RELAX_RATE = 0.25
ECCENTRICITY_SQUARED = 4.0
CORIOLIS_TOP = 1.0
STRENGTH_DECAY = 20.0

MESH = pl.DeviceIdType.MESH
LANES = 128
TINY = 1.1754944e-38
GAIN = 1.0 + RELAX_RATE

MARGIN = SUBCYCLES
EXTRA = 8
PAD = 8
CHUNK = 64
STEP = 32

PACKED = (
    ("u", MARGIN + 1), ("v", MARGIN + 1), ("plus", MARGIN), ("minus", MARGIN), ("twice", MARGIN),
    ("pressure", MARGIN), ("inertia", MARGIN),
    ("ge", MARGIN), ("gn", MARGIN), ("ce", MARGIN), ("cn", MARGIN),
)
WHOLE = 7
OFFSETS = []
for _i, (_, _w) in enumerate(PACKED):
    if _i == 0 or _i == WHOLE:
        OFFSETS.append(0)
    else:
        OFFSETS.append(OFFSETS[-1] + PACKED[_i - 1][1])
HALF = LANES // 2

OWN = 36
AT_RIGHT = 48
AT_HALO = AT_RIGHT + OWN
AT_LEFT = LANES - MARGIN

MAIN_FIELDS = (
    "u", "v", "plus", "minus", "twice", "pressure", "inertia", "turning",
    "ge", "gn", "ce", "cn", "bound", "re", "rn",
    "u_next", "v_next", "e_near", "n_near", "e_back", "n_back",
)


def lane_index(rows):
    return lax.broadcasted_iota(jnp.int32, (rows, LANES), 1)


def rolled(value, shift):
    shift = shift % LANES
    return value if shift == 0 else pltpu.roll(value, shift, 1)


def step_kernel(sizes, *refs):
    gx_count, gy_count, ens_count = sizes
    inputs, refs = refs[:9], refs[9:]
    (vel_out, stress_out, conc_out, landing), refs = refs[:4], refs[4:]
    arrays, refs = refs[: len(MAIN_FIELDS)], refs[len(MAIN_FIELDS) :]
    (svel, sstress, sthick, sconc, smass, swind, scur, smask, sice, expand), refs = refs[:10], refs[10:]
    (out_a, out_b, in_a, in_b, load_sem, send_y, recv_y, send_x, recv_x, send_d, recv_d, send_e, recv_e) = refs
    field = dict(zip(MAIN_FIELDS, arrays))
    stages = (svel, sstress, sthick, sconc, smass, swind, scur, smask)
    rows, cols = conc_out.shape
    main = cols // LANES
    tiles = main + 1
    blocks = rows // BLOCK
    half_rows = rows // 2
    reach = half_rows + 2 * MARGIN
    bases = (PAD, 3 * PAD + reach)
    first_rows = (-MARGIN, half_rows - MARGIN)
    spare = 5 * PAD + 2 * reach
    gx, gy, me = lax.axis_index("gx"), lax.axis_index("gy"), lax.axis_index("ens")
    right, left = lax.rem(gx + 1, gx_count), lax.rem(gx + gx_count - 1, gx_count)
    has_lo, has_hi = gy > 0, gy < gy_count - 1
    lower, upper = jnp.maximum(gy - 1, 0), jnp.minimum(gy + 1, gy_count - 1)
    peers = [lax.rem(me + step, ens_count) for step in range(1, ens_count)]

    barrier = pltpu.get_barrier_semaphore()

    def greet(**where):
        pl.semaphore_signal(barrier, inc=1, device_id=where, device_id_type=MESH)

    greet(gx=left)
    greet(gx=right)
    for peer in peers:
        greet(ens=peer)
    for there, row in ((has_lo, lower), (has_hi, upper)):
        @pl.when(there)
        def _(row=row):
            greet(gy=row)
            greet(gy=row, gx=left)
            greet(gy=row, gx=right)

    def at_rows(ref, where):
        return ref.at[:, where] if len(ref.shape) == 3 else ref.at[where]

    loads = [[
        pltpu.make_async_copy(
            at_rows(source, slice(half * half_rows, (half + 1) * half_rows)),
            at_rows(stage, slice(MARGIN + half * half_rows, MARGIN + (half + 1) * half_rows)),
            load_sem.at[8 * half + number],
        )
        for number, (source, stage) in enumerate(zip(inputs, stages))
    ] for half in range(2)]
    loads[0].append(pltpu.make_async_copy(inputs[8], sice.at[blocks : 2 * blocks], load_sem.at[16]))
    for each in loads[0] + loads[1]:
        each.start()

    def remote(source, target, sends, receives, number, where):
        return pltpu.make_async_remote_copy(
            src_ref=source, dst_ref=target, send_sem=sends.at[number], recv_sem=receives.at[number],
            device_id=where, device_id_type=MESH,
        )

    down, up = [], []
    for number, (source, stage) in enumerate(zip(inputs, stages)):
        extra = EXTRA if number in (0, 7) else 0
        down.append(remote(
            at_rows(source, slice(0, MARGIN + extra)),
            at_rows(stage, slice(MARGIN + rows, 2 * MARGIN + rows + extra)),
            send_y, recv_y, number, {"gy": lower},
        ))
        up.append(remote(
            at_rows(source, slice(rows - MARGIN, rows)),
            at_rows(stage, slice(0, MARGIN)),
            send_y, recv_y, 9 + number, {"gy": upper},
        ))
    down.append(remote(inputs[8], sice.at[2 * blocks : 3 * blocks], send_y, recv_y, 8, {"gy": lower}))
    up.append(remote(inputs[8], sice.at[0:blocks], send_y, recv_y, 17, {"gy": upper}))

    others = has_lo.astype(jnp.int32) + has_hi.astype(jnp.int32)
    pl.semaphore_wait(barrier, 2 + (ens_count - 1) + 3 * others)

    @pl.when(has_lo)
    def _():
        for each in down:
            each.start()

    @pl.when(has_hi)
    def _():
        for each in up:
            each.start()

    block_cols = sice.shape[1]
    spread = (
        lax.broadcasted_iota(jnp.int32, (block_cols, cols), 1) // BLOCK
        == lax.broadcasted_iota(jnp.int32, (block_cols, cols), 0)
    ).astype(jnp.float32)

    repeat = (
        lax.broadcasted_iota(jnp.int32, (8 * blocks, blocks), 0) // 8
        == lax.broadcasted_iota(jnp.int32, (8 * blocks, blocks), 1)
    ).astype(jnp.float32)

    def expand_ice(part):
        flags = sice[part * blocks : (part + 1) * blocks].astype(jnp.float32)
        flags = jnp.dot(repeat, flags, preferred_element_type=jnp.float32)
        expand[8 * part * blocks : 8 * (part + 1) * blocks] = jnp.dot(
            flags, spread, preferred_element_type=jnp.float32)

    def convert(start, count, ice_row, target):
        at = pl.ds(start, count)
        to = pl.ds(target, count)
        row = lax.broadcasted_iota(jnp.int32, (count, LANES), 0) + (gy * rows + (start - MARGIN))
        coriolis = CORIOLIS_TOP * (row.astype(jnp.float32) + 0.5) / (rows * gy_count)
        sent = []
        for t in range(main):
            c = slice(t * LANES, (t + 1) * LANES)
            present = jnp.concatenate([expand[pl.ds(ice_row, 8), c]] * (count // 8))
            alive = smask[at, c].astype(jnp.float32) * present
            one, two = sstress[0, at, c], sstress[1, at, c]
            factor = RELAX_RATE * 0.5 / GAIN
            heavy = smass[at, c]
            heavy = jnp.where(heavy == 0.0, 1.0, heavy)
            turn = coriolis * heavy
            ce, cn = scur[0, at, c], scur[1, at, c]
            value = {
                "u": svel[0, at, c] * alive,
                "v": svel[1, at, c] * alive,
                "plus": one + two,
                "minus": one - two,
                "twice": 2.0 * sstress[2, at, c],
                "pressure": factor * sthick[at, c] * jnp.exp(-STRENGTH_DECAY * (1.0 - sconc[at, c])),
                "inertia": heavy / TIME_STEP,
                "turning": turn,
                "bound": jnp.where(alive == 0.0, jnp.inf, turn * turn),
                "ge": swind[0, at, c] + turn * cn,
                "gn": swind[1, at, c] - turn * ce,
                "ce": alive * ce,
                "cn": alive * cn,
            }
            value["re"], value["rn"] = value["u"] - value["ce"], value["v"] - value["cn"]
            for name, each in value.items():
                field[name][t, to] = each
            value["inertia"] = value["inertia"] * alive
            sent.append(value)
        return sent

    whole, part = range(WHOLE), range(WHOLE, len(PACKED))

    def packed(sent, fields, shift, east, west):
        lanes = lane_index(east.shape[0])
        for number in fields:
            name, width = PACKED[number]
            start = OFFSETS[number] + shift
            here = jnp.logical_and(lanes >= start, lanes < start + width)
            east = jnp.where(here, rolled(sent[main - 1][name], start - (LANES - MARGIN)), east)
            west = jnp.where(here, rolled(sent[0][name], start), west)
        return east, west

    own_at = (PAD + MARGIN, bases[1] + MARGIN)
    for half in range(2):
        for each in loads[half]:
            each.wait()
        if half == 0:
            expand_ice(1)

        def convert_own(block, _, half=half):
            start = pl.multiple_of(half * half_rows + block * BLOCK, 8)
            sent = convert(
                MARGIN + start, BLOCK, pl.multiple_of(8 * (blocks + half * blocks // 2 + block), 8),
                pl.multiple_of(own_at[half] + block * BLOCK, 8),
            )
            zero = jnp.zeros((BLOCK, LANES), jnp.float32)
            to, to_half = pl.ds(start, BLOCK), pl.ds(pl.multiple_of(block * BLOCK, 8), BLOCK)
            out_a[0, to], out_a[1, to] = packed(sent, whole, 0, zero, zero)
            before = (out_b[0, to_half], out_b[1, to_half]) if half else (zero, zero)
            out_b[0, to_half], out_b[1, to_half] = packed(sent, part, half * HALF, *before)
            return 0

        lax.fori_loop(0, blocks // 2, convert_own, 0)

    def message(name, tile, at):
        value = field[name][tile, at]
        return jnp.where(field["bound"][tile, at] == jnp.inf, 0.0, value) if name == "inertia" else value

    sides = (right, left)
    across, corner_lo, corner_hi = [], [], []
    for side, to in enumerate(sides):
        across.append(remote(
            out_a.at[side], in_a.at[side, MARGIN : MARGIN + rows], send_x, recv_x, 2 * side, {"gx": to}))
        across.append(remote(
            out_b.at[side], in_b.at[side, MARGIN : MARGIN + half_rows], send_x, recv_x, 2 * side + 1, {"gx": to}))
        lo, hi = {"gx": to, "gy": lower}, {"gx": to, "gy": upper}
        corner_lo.append(remote(
            out_a.at[side, 0 : MARGIN + EXTRA],
            in_a.at[side, MARGIN + rows : 2 * MARGIN + rows + EXTRA],
            send_d, recv_d, 4 * side, lo))
        corner_lo.append(remote(
            out_b.at[side, 0:MARGIN],
            in_b.at[side, MARGIN + half_rows : 2 * MARGIN + half_rows],
            send_d, recv_d, 4 * side + 1, lo))
        corner_hi.append(remote(
            out_a.at[side, rows - MARGIN : rows], in_a.at[side, 0:MARGIN],
            send_d, recv_d, 4 * side + 2, hi))
        corner_hi.append(remote(
            out_b.at[side, half_rows - MARGIN : half_rows], in_b.at[side, 0:MARGIN],
            send_d, recv_d, 4 * side + 3, hi))
    for each in across:
        each.start()

    @pl.when(has_lo)
    def _():
        for each in corner_lo:
            each.start()

    @pl.when(has_hi)
    def _():
        for each in corner_hi:
            each.start()

    convert(MARGIN + half_rows, MARGIN, 8 * (blocks + blocks // 2), own_at[0] + half_rows)
    convert(half_rows, MARGIN, 8 * (blocks + blocks // 2 - 1), bases[1])

    def strip_columns(target, count):
        at = pl.ds(target, count)
        lanes = lane_index(count)
        for name, _ in PACKED:
            field[name][main, at] = jnp.where(
                lanes < OWN, message(name, 0, at), rolled(message(name, main - 1, at), AT_HALO - LANES))

    for half in range(2):
        def own_columns(block, _, half=half):
            strip_columns(pl.multiple_of(own_at[half] + block * CHUNK, 8), CHUNK)
            return 0

        lax.fori_loop(0, half_rows // CHUNK, own_columns, 0, unroll=True)
    strip_columns(own_at[0] + half_rows, MARGIN)
    strip_columns(bases[1], MARGIN)

    @pl.when(has_lo)
    def _():
        for each in up:
            each.wait_recv()

    @pl.when(jnp.logical_not(has_lo))
    def _():
        for stage in stages:
            for index in range(stage.shape[0]) if len(stage.shape) == 3 else (None,):
                view = stage if index is None else stage.at[index]
                view[0:MARGIN] = jnp.zeros((MARGIN, cols), stage.dtype)
        sice[0:blocks] = jnp.zeros((blocks, block_cols), jnp.int32)

    @pl.when(has_hi)
    def _():
        for each in down:
            each.wait_recv()

    @pl.when(jnp.logical_not(has_hi))
    def _():
        for stage in stages:
            count = stage.shape[-2] - MARGIN - rows
            for index in range(stage.shape[0]) if len(stage.shape) == 3 else (None,):
                view = stage if index is None else stage.at[index]
                view[MARGIN + rows : MARGIN + rows + count] = jnp.zeros((count, cols), stage.dtype)
        sice[2 * blocks : 3 * blocks] = jnp.zeros((blocks, block_cols), jnp.int32)

    expand_ice(0)
    expand_ice(2)
    convert(0, MARGIN, 8 * (blocks - 1), bases[0])
    convert(MARGIN + rows, MARGIN, 16 * blocks, own_at[1] + half_rows)
    beyond = slice(2 * MARGIN + rows, 2 * MARGIN + rows + EXTRA)
    past = slice(bases[1] + reach, bases[1] + reach + EXTRA)
    other_past = slice(bases[0] + reach, bases[0] + reach + EXTRA)
    for t in range(main):
        c = slice(t * LANES, (t + 1) * LANES)
        alive = smask[beyond, c].astype(jnp.float32) * expand[16 * blocks : 16 * blocks + 8, c]
        field["u"][t, past] = svel[0, beyond, c] * alive
        field["v"][t, past] = svel[1, beyond, c] * alive

    for each in across:
        each.wait_recv()

    @pl.when(has_lo)
    def _():
        for each in corner_hi:
            each.wait_recv()

    @pl.when(jnp.logical_not(has_lo))
    def _():
        for side in range(2):
            in_a[side, 0:MARGIN] = jnp.zeros((MARGIN, LANES), jnp.float32)
            in_b[side, 0:MARGIN] = jnp.zeros((MARGIN, LANES), jnp.float32)

    @pl.when(has_hi)
    def _():
        for each in corner_lo:
            each.wait_recv()

    @pl.when(jnp.logical_not(has_hi))
    def _():
        for side in range(2):
            in_a[side, MARGIN + rows :] = jnp.zeros((MARGIN + EXTRA, LANES), jnp.float32)
            in_b[side, MARGIN + half_rows :] = jnp.zeros((MARGIN, LANES), jnp.float32)

    def strip_value(number, row, target, count, half_start, half_lane):
        name, width = PACKED[number]
        lanes = lane_index(count)
        if number < WHOLE:
            arrived, there, lane = in_a, pl.ds(row + MARGIN, count), OFFSETS[number]
        else:
            arrived, there, lane = in_b, pl.ds(half_start, count), OFFSETS[number] + half_lane
        value = jnp.where(lanes < AT_HALO + width, rolled(arrived[1, there], AT_HALO - lane), 0.0)
        value = jnp.where(lanes < AT_HALO, field[name][main, pl.ds(target, count)], value)
        return jnp.where(lanes >= AT_LEFT, rolled(arrived[0, there], AT_LEFT - lane), value)

    def strip_rows(first, target, count, half_start, half_lane):
        at = pl.ds(target, count)
        value = {
            name: strip_value(number, first, target, count, half_start, half_lane)
            for number, (name, _) in enumerate(PACKED)
        }
        row = lax.broadcasted_iota(jnp.int32, (count, LANES), 0) + (gy * rows + first)
        coriolis = CORIOLIS_TOP * (row.astype(jnp.float32) + 0.5) / (rows * gy_count)
        empty = value["inertia"] == 0.0
        heavy = jnp.where(empty, 1.0 / TIME_STEP, value["inertia"])
        value["inertia"] = heavy
        value["turning"] = coriolis * (heavy * TIME_STEP)
        value["bound"] = jnp.where(empty, jnp.inf, value["turning"] * value["turning"])
        value["re"], value["rn"] = value["u"] - value["ce"], value["v"] - value["cn"]
        for name, each in value.items():
            field[name][main, at] = each

    for half in range(2):
        def strip_own(block, _, half=half):
            start = pl.multiple_of(block * CHUNK, 8)
            strip_rows(half * half_rows + start, pl.multiple_of(own_at[half] + start, 8), CHUNK,
                       MARGIN + start, half * HALF)
            return 0

        lax.fori_loop(0, half_rows // CHUNK, strip_own, 0, unroll=True)
    strip_rows(half_rows, own_at[0] + half_rows, MARGIN, MARGIN, HALF)
    strip_rows(half_rows - MARGIN, bases[1], MARGIN, half_rows, 0)
    strip_columns(bases[0], MARGIN)
    strip_columns(own_at[1] + half_rows, MARGIN)
    strip_rows(-MARGIN, bases[0], MARGIN, 0, HALF)
    strip_rows(rows, own_at[1] + half_rows, MARGIN, MARGIN + half_rows, 0)
    for number in range(2):
        name = PACKED[number][0]
        lanes = lane_index(EXTRA)
        field[name][main, past] = jnp.where(
            lanes < OWN, field[name][0, past], rolled(field[name][main - 1, past], AT_HALO - LANES))
        field[name][main, past] = strip_value(number, rows + MARGIN, past.start, EXTRA, 0, 0)
        for t in range(tiles):
            field[name][t, other_past] = field[name][t, bases[1] + 2 * MARGIN : bases[1] + 2 * MARGIN + EXTRA]
    for name in ("plus", "minus", "twice"):
        for t in range(tiles):
            for base in bases:
                field[name][t, base - PAD : base] = jnp.zeros((PAD, LANES), jnp.float32)

    u, v, plus, minus, twice = (field[name] for name in ("u", "v", "plus", "minus", "twice"))
    u_next, v_next = field["u_next"], field["v_next"]
    def ahead(values):
        turned = [rolled(value, -1) for value in values]
        at_end = lane_index(values[0].shape[0]) == LANES - 1
        return [jnp.where(at_end, turned[(t + 1) % main], turned[t]) for t in range(main)] + turned[main:]

    def behind(values):
        turned = [rolled(value, 1) for value in values]
        at_start = lane_index(values[0].shape[0]) == 0
        return [jnp.where(at_start, turned[t - 1 if t else main - 1], turned[t]) for t in range(main)] + turned[main:]

    def gradients(start, count):
        add, sub, add_s, sub_s = [], [], [], []
        at, after = pl.ds(start, count), pl.ds(start + 1, count)
        for t in range(tiles):
            u0, u1, v0, v1 = u[t, at], u[t, after], v[t, at], v[t, after]
            a, b, c, d = u0 + u1, u1 - u0, v0 + v1, v1 - v0
            add.append(a + d)
            sub.append(a - d)
            add_s.append(b + c)
            sub_s.append(b - c)
        return add, sub, add_s, sub_s

    def stress_sums(start):
        at, before = pl.ds(start, STEP), pl.ds(start - 1, STEP)
        e_near, e_far, n_near, n_far = [], [], [], []
        for t in range(tiles):
            p1, p0 = plus[t, at], plus[t, before]
            m1, m0 = minus[t, at], minus[t, before]
            s1, s0 = twice[t, at], twice[t, before]
            a, d, b, e = p0 + p1, s1 - s0, s0 + s1, m1 - m0
            e_near.append(a + d)
            e_far.append(a - d)
            n_near.append(b + e)
            n_far.append(b - e)
        return e_near, e_far, n_near, n_far

    def stress_rows(start, growth):
        for t, piece in [(t, piece) for t in range(tiles) for piece in range(0, STEP, 8)]:
            at, after = pl.ds(start + piece, 8), pl.ds(start + piece + 1, 8)
            u0, u1, v0, v1 = u[t, at], u[t, after], v[t, at], v[t, after]
            u2, u3, v2, v3 = u_next[t, at], u_next[t, after], v_next[t, at], v_next[t, after]
            along, across_y = (u2 + u3) - (u0 + u1), (v1 - v0) + (v3 - v2)
            div, tension = along + across_y, along - across_y
            shear = ((u1 - u0) + (u3 - u2)) + ((v2 + v3) - (v0 + v1))
            square = div * div + (1.0 / ECCENTRICITY_SQUARED) * (tension * tension + shear * shear)
            inverse = lax.rsqrt(jnp.maximum(square, TINY))
            weight = (field["pressure"][t, at] * growth) * jnp.minimum(inverse, 1.0)
            quarter = weight * (1.0 / ECCENTRICITY_SQUARED)
            change = weight * (div - square * inverse)
            other = quarter * tension
            plus[t, at] = plus[t, at] + (change + other)
            minus[t, at] = minus[t, at] + (change - other)
            twice[t, at] = twice[t, at] + quarter * shear

    def velocity_rows(start, scale):
        for t, piece in [(t, piece) for t in range(tiles) for piece in range(0, STEP, 8)]:
            at = pl.ds(start + piece, 8)
            de, dn = field["re"][t, at], field["rn"][t, at]
            square = de * de + dn * dn
            drag = square * lax.rsqrt(jnp.maximum(square, TINY))
            heavy, turn = field["inertia"][t, at], field["turning"][t, at]
            diag = heavy + drag
            force_e = (field["e_near"][t, at] - field["e_back"][t, at]) * scale
            force_n = (field["n_near"][t, at] - field["n_back"][t, at]) * scale
            push_e = heavy * de + (force_e + field["ge"][t, at])
            push_n = heavy * dn + (force_n + field["gn"][t, at])
            inverse = lax.rsqrt(diag * diag + field["bound"][t, at])
            inverse = inverse * inverse
            de = (diag * push_e + turn * push_n) * inverse
            dn = (diag * push_n - turn * push_e) * inverse
            field["re"][t, at], field["rn"][t, at] = de, dn
            u[t, at] = de + field["ce"][t, at]
            v[t, at] = dn + field["cn"][t, at]

    def run(count, base, carried):
        last = base + reach - STEP

        def step(_, carried):
            at_g, at_h, at_s, at_f, at_v, growth, growth_h, growth_s, scale, scale_h, scale_s, scale_f, scale_v = carried
            at_g, at_h, at_s, at_f, at_v = (pl.multiple_of(each, 8) for each in (at_g, at_h, at_s, at_f, at_v))

            def keep(names, values, start):
                for name, each in zip(names, values):
                    for t in range(tiles):
                        field[name][t, pl.ds(start, STEP)] = each[t]

            moved = [ahead([ref[t, pl.ds(at_g, STEP)] for t in range(tiles)]) for ref in (u, v)]
            e_near, e_far, n_near, n_far = stress_sums(at_f)
            e_back, n_back = behind(e_far), behind(n_far)
            stress_rows(at_s, growth_s)
            velocity_rows(at_v, scale_v)
            keep(("u_next", "v_next"), moved, at_g)
            keep(("e_near", "n_near", "e_back", "n_back"), (e_near, n_near, e_back, n_back), at_f)
            wrap = at_g == last
            return (
                jnp.where(wrap, base, jnp.where(at_g == spare, spare, at_g + STEP)), at_g, at_h, at_s, at_f,
                jnp.where(wrap, growth * GAIN, growth), growth, growth_h,
                jnp.where(wrap, scale * (1.0 / GAIN), scale), scale, scale_h, scale_s, scale_f,
            )

        return lax.fori_loop(0, count, step, carried)

    def begin(at, carried):
        growth, scale = jnp.float32(GAIN), jnp.float32(0.25 / GAIN)
        return (jnp.int32(at),) + carried[1:5] + (growth,) + carried[6:8] + (scale,) + carried[9:]

    shrink = 0.5 * GAIN**-SUBCYCLES

    def merged(values):
        lanes = lane_index(values[0].shape[0])
        on_left, on_right = lanes < MARGIN, lanes >= LANES - MARGIN - 2
        values = list(values)
        values[0] = jnp.where(on_left, values[main], values[0])
        values[main - 1] = jnp.where(on_right, rolled(values[main], LANES - AT_HALO), values[main - 1])
        return values[:main]

    def finish_conc(start, row, count):
        add, sub, _, _ = gradients(start, count)
        add_next = ahead(add)
        div = merged([add_next[t] - sub[t] for t in range(tiles)])
        for t in range(main):
            c = slice(t * LANES, (t + 1) * LANES)
            value = sconc[pl.ds(MARGIN + row, count), c]
            conc_out[pl.ds(row, count), c] = jnp.clip(value - value * (0.5 * div[t]), 0.0, 1.0)

    def finish(start, row, count):
        here, at = pl.ds(start, count), pl.ds(row, count)
        east, north, one, two, three = (
            merged([ref[t, here] for t in range(tiles)]) for ref in (u, v, plus, minus, twice)
        )
        for t in range(main):
            c = slice(t * LANES, (t + 1) * LANES)
            vel_out[0, at, c] = east[t]
            vel_out[1, at, c] = north[t]
            stress_out[0, at, c] = (one[t] + two[t]) * shrink
            stress_out[1, at, c] = (one[t] - two[t]) * shrink
            stress_out[2, at, c] = three[t] * shrink
        finish_conc(start, row, count)

    def finish_half(half):
        def body(block, _):
            start = block * CHUNK
            finish(
                pl.multiple_of(jnp.where(half == 0, own_at[0], own_at[1]) + start, 8),
                pl.multiple_of(half * half_rows + start, 8), CHUNK,
            )
            return 0

        lax.fori_loop(0, half_rows // CHUNK, body, 0, unroll=True)

    early = (1 - me) if ens_count == 2 else jnp.int32(0)
    late = 1 - early
    share = rows // ens_count
    swaps = []
    for step, peer in enumerate(peers):
        part_of = pl.ds(pl.multiple_of(peer * share, 8), share)
        swaps.append(remote(
            vel_out.at[:, part_of], landing.at[step, 1:3], send_e, recv_e, 2 * step, {"ens": peer}))
        swaps.append(remote(
            conc_out.at[part_of], landing.at[step, 0], send_e, recv_e, 2 * step + 1, {"ens": peer}))

    for beyond_domain in (past, other_past):
        for ref, target in ((u, u_next), (v, v_next)):
            for t, each in enumerate(ahead([ref[t, beyond_domain] for t in range(tiles)])):
                target[t, beyond_domain] = each
    steps, lag = SUBCYCLES * (reach // STEP), 4
    one, empty = jnp.float32(1.0), jnp.int32(spare)
    first = jnp.where(early == 0, bases[0], bases[1])
    second = jnp.where(late == 0, bases[0], bases[1])
    carried = begin(first, (empty,) * 5 + (one,) * 8)
    carried = run(steps, first, carried)
    carried = run(lag, second, begin(second, carried))
    finish_half(early)
    if ens_count == 2:
        for each in swaps:
            each.start()
    carried = run(steps - lag, second, carried)
    run(lag, spare, begin(spare, carried))
    finish_half(late)
    if ens_count != 2:
        for each in swaps:
            each.start()
    for each in across:
        each.wait_send()

    @pl.when(has_lo)
    def _():
        for each in down + corner_lo:
            each.wait_send()

    @pl.when(has_hi)
    def _():
        for each in up + corner_hi:
            each.wait_send()

    for each in swaps:
        each.wait_recv()
    for each in swaps:
        each.wait_send()


def write_kernel(count, vel, stress, conc, landing, vel_out, stress_out, mean_out, spread_out, mean, spread, sems):
    copies = [
        pltpu.make_async_copy(vel, vel_out, sems.at[0]),
        pltpu.make_async_copy(stress, stress_out, sems.at[1]),
    ]
    for each in copies:
        each.start()
    share = mean.shape[1]
    own = pl.ds(pl.multiple_of(lax.axis_index("ens") * share, 8), share)
    for f in range(3):
        values = [conc[own] if f == 0 else vel[f - 1, own]]
        values += [landing[step, f] for step in range(count - 1)]
        average = functools.reduce(jnp.add, values) / count
        mean[f] = average
        spread[f] = functools.reduce(jnp.add, [(v - average) * (v - average) for v in values]) / count
    more = [
        pltpu.make_async_copy(mean, mean_out, sems.at[2]),
        pltpu.make_async_copy(spread, spread_out, sems.at[3]),
    ]
    for each in more:
        each.start()
    for each in copies + more:
        each.wait()


def solution(mesh):
    gx_count, gy_count, ens_count = mesh.shape["gx"], mesh.shape["gy"], mesh.shape["ens"]
    f32 = jnp.float32

    def vmem(*shape, dtype=f32):
        return pltpu.VMEM(shape, dtype)

    def specs(count, space):
        return [pl.BlockSpec(memory_space=space)] * count

    def body(velocity, stress, thickness, concentration, node_mass, wind, current, mask, ice):
        rows, cols = mask.shape
        share = rows // ens_count
        tiles = cols // LANES + 1
        block_rows, block_cols = ice.shape[1:]
        tall = rows + 2 * MARGIN
        total = -(-(5 * PAD + 2 * (rows // 2 + 2 * MARGIN) + STEP + PAD) // 32) * 32
        shape = lambda *dims: jax.ShapeDtypeStruct(dims, f32)
        dma = lambda count: pltpu.SemaphoreType.DMA((count,))
        state = pl.pallas_call(
            functools.partial(step_kernel, (gx_count, gy_count, ens_count)),
            name="subcycles",
            out_shape=(
                shape(2, rows, cols),
                shape(3, rows, cols),
                shape(rows, cols),
                shape(ens_count - 1, 3, share, cols),
            ),
            in_specs=specs(9, pltpu.HBM),
            out_specs=tuple(specs(4, pltpu.VMEM)),
            scratch_shapes=[vmem(tiles, total, LANES)] * len(MAIN_FIELDS)
            + [
                vmem(2, tall + EXTRA, cols),
                vmem(3, tall, cols),
                vmem(tall, cols),
                vmem(tall, cols),
                vmem(tall, cols),
                vmem(2, tall, cols),
                vmem(2, tall, cols),
                vmem(tall + EXTRA, cols, dtype=jnp.int32),
                vmem(3 * block_rows, block_cols, dtype=jnp.int32),
                vmem(24 * block_rows, cols),
                vmem(2, rows, LANES),
                vmem(2, rows // 2, LANES),
                vmem(2, tall + EXTRA, LANES),
                vmem(2, rows // 2 + 2 * MARGIN, LANES),
                dma(17), dma(18), dma(18), dma(4), dma(4), dma(8), dma(8),
                dma(2 * (ens_count - 1)), dma(2 * (ens_count - 1)),
            ],
            compiler_params=pltpu.CompilerParams(
                collective_id=0, has_side_effects=True, vmem_limit_bytes=32 << 20),
        )(*(pltpu.with_memory_space_constraint(each, pltpu.HBM) for each in (
            velocity[0], stress[0], thickness[0], concentration[0], node_mass[0], wind[0], current[0], mask, ice[0])))
        vel_out, stress_out, mean, spread = pl.pallas_call(
            functools.partial(write_kernel, ens_count),
            name="write",
            out_shape=(shape(2, rows, cols), shape(3, rows, cols), shape(3, share, cols), shape(3, share, cols)),
            in_specs=specs(4, pltpu.VMEM),
            out_specs=tuple(specs(4, pltpu.HBM)),
            scratch_shapes=[vmem(3, share, cols), vmem(3, share, cols), dma(4)],
            compiler_params=pltpu.CompilerParams(vmem_limit_bytes=4 << 20),
        )(*state)
        return vel_out[None], stress_out[None], mean, spread

    grid = P("ens", "gy", "gx")
    pair = P("ens", None, "gy", "gx")
    split = P(None, ("gy", "ens"), "gx")
    return jax.shard_map(
        body,
        mesh=mesh,
        in_specs=(pair, pair, grid, grid, grid, pair, pair, P("gy", "gx"), grid),
        out_specs=(pair, pair, split, split),
        check_vma=False,
    )
```
